32 devices in a mesh: rows: 8 (over z, x), cols: 4 (over y, core).
Axes of the slice: x: 2, y: 2, z: 4, core: 2. Of those that a mesh axis runs over, the one named last changes fastest.
Arguments:
- matrix: float32 [512, 32, 2, 128], P('rows', 'cols'), may hold values from -54 to 54
- plan: int32 [2, 4, 256], replicated, may hold values from 0 to 255, as said below
Outputs:
- rotated: float32 [512, 32, 2, 128], P('rows', 'cols')
The draws below stay inside these ranges and needn't reach their ends.
Inputs may be any that keep to these rules, and one draw needn't show every extreme that they name: Each plan[s, r] pairs the 256 columns: partner of partner of i is i, and no column is its own partner.
All inputs are finite; a program needn't handle non-finite values.
Results may differ from the reference program's by a relative error of at most 0.0003.
Values sent between devices are 32-bit elements; how exact they have to be, the bound alone decides.
A program may use at most 128 MiB of HBM per device.

```python
import math
import jax
import jax.numpy as jnp
from jax import lax

BLOCK = 128
PAIR_DEV = 8
STEPS = 2
ROUNDS = 4
PAIRS = 32
ROWS = 512


def draw_matrix(key, part):
    base_key = jax.random.fold_in(key, 11)
    first, second, third = jax.random.split(base_key, 3)
    shape = (ROWS, PAIRS, 2, BLOCK)
    row_scale = jnp.exp(jax.random.uniform(second, (ROWS, 1, 1, 1), jnp.float32, math.log(0.3), math.log(3.0)))
    col_scale = jnp.exp(jax.random.uniform(third, (1, PAIRS, 2, BLOCK), jnp.float32, math.log(0.3), math.log(3.0)))
    values = jnp.clip(jax.random.normal(first, shape, jnp.float32), -6.0, 6.0)
    return (values * row_scale * col_scale).astype(jnp.float32)


def draw_plan(key, part):
    width = 2 * BLOCK

    def one_table(inner_key):
        order = jax.random.permutation(inner_key, width).astype(jnp.int32)
        first_half = order[0::2]
        second_half = order[1::2]
        partner = jnp.zeros((width,), jnp.int32).at[first_half].set(second_half).at[second_half].set(first_half)
        return partner
    keys = jax.random.split(jax.random.fold_in(key, 7), STEPS * ROUNDS)
    tables = jax.vmap(one_table)(keys)
    return tables.reshape(STEPS, ROUNDS, width).astype(jnp.int32)


def setup_inputs(seed: int = 0) -> dict:
    streams_of = jax.random.split(jax.random.key(seed), 3)
    return {
        "matrix": draw_matrix(jax.random.fold_in(streams_of[2], 71), 0),
        "plan": draw_plan(jax.random.fold_in(streams_of[2], 71), 0),
    }


def diagonalize(grams, table):
    width = grams.shape[1]
    indices = jnp.arange(width, dtype=jnp.int32)
    rotation = jnp.broadcast_to(jnp.eye(width, dtype=jnp.float32), grams.shape)
    unit_matrix = jnp.eye(width, dtype=jnp.float32)
    for round_index in range(table.shape[0]):
        partner = table[round_index]
        onehot = (partner[:, None] == indices[None, :]).astype(jnp.float32)
        diagonal_now = jnp.diagonal(grams, axis1=1, axis2=2)
        partner_diag = jnp.einsum('pj,ij->pi', diagonal_now, onehot, precision=lax.Precision.HIGHEST)
        partner_gram = lax.optimization_barrier(jnp.sum(grams * onehot[None], axis=2))
        orient = jnp.where(indices < partner, 1.0, -1.0).astype(jnp.float32)
        spread = orient[None, :] * (partner_diag - diagonal_now)
        sign_part = jnp.where(spread >= 0.0, 1.0, -1.0).astype(jnp.float32)
        tangent = sign_part * 2.0 * partner_gram / (jnp.abs(spread) + jnp.sqrt(spread * spread + 4.0 * partner_gram * partner_gram))
        cosine = 1.0 / jnp.sqrt(1.0 + tangent * tangent)
        sine_part = tangent * cosine
        off_part = jnp.swapaxes(onehot[None] * (-orient[None, :] * sine_part)[:, :, None], 1, 2)
        rot_now = cosine[:, :, None] * unit_matrix[None] + off_part
        product = jnp.einsum('pij,pjk->pik', grams, rot_now, precision=lax.Precision.HIGHEST)
        grams = jnp.einsum('pji,pjk->pik', rot_now, product, precision=lax.Precision.HIGHEST)
        rotation = jnp.einsum('pij,pjk->pik', rotation, rot_now, precision=lax.Precision.HIGHEST)
    return (grams, rotation)

def reference(matrix, plan):
    rows_all, pairs, halves, width = matrix.shape
    columns = matrix.reshape(rows_all, pairs, halves * width)
    for step_index in range(STEPS):
        grams = jnp.einsum('mpi,mpj->pij', columns, columns, precision=lax.Precision.HIGHEST)
        grams, rotation = diagonalize(grams, plan[step_index])
        columns = jnp.einsum('mpi,pij->mpj', columns, rotation, precision=lax.Precision.HIGHEST)
        quarter = columns.reshape(rows_all, pairs, halves, width)
        tops = quarter[:, :, 0, :]
        bottoms = jnp.roll(quarter[:, :, 1, :], PAIR_DEV, axis=1)
        columns = jnp.stack([tops, bottoms], axis=2).reshape(rows_all, pairs, halves * width)
    return columns.reshape(matrix.shape)
```

```python
import functools

import jax
import jax.numpy as jnp
from jax import lax
from jax.experimental import pallas as pl
from jax.experimental.pallas import tpu as pltpu
from jax.sharding import PartitionSpec as P

MESH = pl.DeviceIdType.MESH
NN = (((1,), (0,)), ((), ()))
NT = (((1,), (1,)), ((), ()))
F32 = jnp.float32
BF16 = jnp.bfloat16


def dot(a, b, dims=NN, precision=None):
    return lax.dot_general(a, b, dims, precision=precision, preferred_element_type=F32)


def exact_dot(a, b, dims=NN):
    return dot(a, b, dims, lax.Precision.HIGHEST)


def moved_columns(a, onehot):
    hi = a.astype(BF16)
    rest = a - hi.astype(F32)
    mid = rest.astype(BF16)
    lo = (rest - mid.astype(F32)).astype(BF16)
    return dot(hi, onehot) + dot(mid, onehot) + dot(lo, onehot)


def moved_columns_short(a, onehot):
    hi = a.astype(BF16)
    mid = (a - hi.astype(F32)).astype(BF16)
    return dot(hi, onehot) + dot(mid, onehot)


def gathered_columns(a, source):
    rows, width = a.shape
    half = width // 2
    parts = []
    for h in range(2):
        index = source[:, h * half:(h + 1) * half]
        lane = jnp.broadcast_to(index % half, (rows, half))
        second = jnp.broadcast_to(index >= half, (rows, half))
        left, right = (
            jnp.take_along_axis(a[:, k * half:(k + 1) * half], lane, axis=1, mode="promise_in_bounds") for k in range(2))
        parts.append(jnp.where(second, right, left))
    return jnp.concatenate(parts, axis=1)


def rotated_columns(a, cosine, sine):
    half = a.shape[-1] // 2
    left, right = a[..., :half], a[..., half:]
    return jnp.concatenate([cosine * left - sine * right, sine * left + cosine * right], axis=-1)


def folded(a):
    return jnp.sum(a.reshape(-1, 8, a.shape[-1]), axis=0)


def products(factors):
    low = high = cross = 0.0
    for a, b in factors:
        half = a.shape[1] // 2
        low = low + folded(a[:, :half] * b[:, :half])
        high = high + folded(a[:, half:] * b[:, half:])
        cross = cross + folded(a[:, :half] * b[:, half:])
    return low, high, cross


def angles(sums):
    low, high, cross = (jnp.sum(v, axis=0, keepdims=True) for v in sums)
    spread = high - low
    sign = jnp.where(spread >= 0.0, 1.0, -1.0)
    root = jnp.sqrt(spread * spread + 4.0 * cross * cross)
    tangent = sign * 2.0 * cross / (jnp.abs(spread) + root)
    cosine = 1.0 / jnp.sqrt(1.0 + tangent * tangent)
    return cosine, tangent * cosine


def orders(partner):
    width = partner.shape[1]
    shape = (width, width)
    row = lax.broadcasted_iota(jnp.int32, shape, 0)
    col = lax.broadcasted_iota(jnp.int32, shape, 1)
    other = jnp.broadcast_to(partner, shape)
    swap = row == other
    one = jnp.ones(shape, BF16)

    def bits(mask):
        return jnp.where(mask, 1.0, 0.0).astype(BF16)

    swap_b = bits(swap)
    first_row = other > col
    rank_row = dot(bits(first_row), bits(row < col))
    mate_row = dot(rank_row.astype(BF16), swap_b)
    place_row = jnp.where(first_row, rank_row, mate_row + float(width // 2))
    first_col = dot(bits(swap & (col > row)), one) > 0.5
    rank_col = dot(bits(col < row), bits(first_col))
    mate_col = dot(swap_b, rank_col.astype(BF16))
    place_col = jnp.where(first_col, rank_col, mate_col + float(width // 2))
    forward = bits(place_col == col.astype(F32))
    backward = bits(place_row == row.astype(F32))
    return forward, backward


def kernel(sizes, x_hbm, plan_hbm, out_ref, x_ref, plan_ref, stage, held, state, bottoms, landed, tops, row_state,
           row_tops, row_low, row_landed, turns, moves, sources, grams, load_sem, in_send, in_recv, mid_send, mid_recv,
           gram_send, gram_recv, turn_send, turn_recv, row_send, row_recv):
    owners, groups, cols, rows_here, steps, rounds, width = sizes
    half = width // 2
    rows_all = owners * rows_here
    me = lax.axis_index("rows")
    col = lax.axis_index("cols")
    group, mine = me // owners, me % owners
    right = (col + 1) % cols

    def at(owner_shift, col_shift=0, group_shift=0):
        row = ((group + group_shift) % groups) * owners + (mine + owner_shift) % owners
        return row, (col + col_shift) % cols

    peers = {(o, 0, 0) for o in range(owners)} | {(0, c, 0) for c in (1, cols - 1)} | {(0, 0, g) for g in range(groups)}
    peers = sorted(peers - {(0, 0, 0)})
    barrier = pltpu.get_barrier_semaphore()
    for peer in peers:
        pl.semaphore_signal(barrier, inc=1, device_id=at(*peer), device_id_type=MESH)
    load = pltpu.make_async_copy(x_hbm, x_ref, load_sem.at[0])
    load.start()
    load_plan = pltpu.make_async_copy(plan_hbm, plan_ref, load_sem.at[1])
    load_plan.start()
    load.wait()
    for k in range(owners):
        for h in range(2):
            stage[k, :, h * half:(h + 1) * half] = x_ref[pl.ds(2 * k + h, rows_here, stride=2 * owners), :]
    with jax.named_scope("barrier_wait"):
        pl.semaphore_wait(barrier, len(peers))

    def rows_of(owner):
        return pl.ds(pl.multiple_of(owner * rows_here, rows_here), rows_here)

    incoming = []
    for d in range(1, owners):
        copy = pltpu.make_async_remote_copy(
            stage.at[(mine + d) % owners], held.at[rows_of(mine), :], in_send.at[d], in_recv.at[d],
            device_id=at(d), device_id_type=MESH)
        copy.start()
        incoming.append(copy)

    load_plan.wait()
    with jax.named_scope("orders"):
        ladder = lax.broadcasted_iota(jnp.int32, (8, width), 1).astype(F32).astype(BF16)
        for s in range(steps):
            before = None
            for r in range(rounds + 1):
                if r < rounds:
                    forward, backward = orders(plan_ref[s, r:r + 1, :])
                    move = forward if r == 0 else dot(before, forward).astype(BF16)
                    before = backward
                else:
                    move = before
                moves[s, r] = move
                sources[s, r] = dot(ladder, move).astype(jnp.int32)

    def advanced(ref, turn, s, r):
        parts = []
        cut = ref.shape[0] // 2
        for h in range(2):
            part = ref[h * cut:(h + 1) * cut, :]
            if turn is not None:
                part = rotated_columns(part, *turn)
            if h == 0:
                parts.append(moved_columns(part, moves[s, r]))
            else:
                parts.append(gathered_columns(part, sources[s, r, 0:1, :]))
        return parts

    def kept(ref, parts):
        cut = ref.shape[0] // 2
        for h in range(2):
            ref[h * cut:(h + 1) * cut, :] = parts[h]

    def tell(s, r, turn):
        cosine, sine = turn
        turns[s, r, mine] = jnp.concatenate([cosine, sine], axis=0)
        told = []
        for d in range(1, owners):
            copy = pltpu.make_async_remote_copy(
                turns.at[s, r, mine], turns.at[s, r, mine], turn_send.at[s, r, d], turn_recv.at[s, r, d],
                device_id=at(d), device_id_type=MESH)
            copy.start()
            told.append(copy)
        return told

    def solved(s, sums):
        if sums is None:
            x = tops[...]
            gram = exact_dot(x.T, x)
            grams[s, group] = gram
            shared = []
            for g in range(1, groups):
                copy = pltpu.make_async_remote_copy(
                    grams.at[s, group], grams.at[s, group], gram_send.at[s, g], gram_recv.at[s, g],
                    device_id=at(0, 0, g), device_id_type=MESH)
                copy.start()
                shared.append(copy)
            for copy in shared:
                copy.wait()
            gram = grams[s, 0]
            for g in range(1, groups):
                gram = gram + grams[s, g]
            state[0:width, :] = gram
            shape = (width, width)
            eye = lax.broadcasted_iota(jnp.int32, shape, 0) == lax.broadcasted_iota(jnp.int32, shape, 1)
            state[width:2 * width, :] = jnp.where(eye, 1.0, 0.0)
        turn, all_turns, told = None, [], []
        for r in range(rounds):
            if r > 0 or sums is None:
                parts = advanced(state, turn, s, r)
                kept(state, parts)
                factors = [tuple(parts)] if groups > 1 else [(part, part) for part in parts]
                sums = products(factors)
            turn = angles(sums)
            told.append(tell(s, r, turn))
            all_turns.append(turn)
        return all_turns, told

    def final_parts(s, all_turns):
        if groups > 1:
            turn = None
            for r in range(rounds):
                kept(tops, advanced(tops, turn, s, r))
                turn = all_turns[r]
            return advanced(tops, turn, s, rounds)
        return advanced(state, all_turns[-1], s, rounds)

    chunks = 2 if owners % 2 == 0 else 1
    size = owners // chunks

    def short_moved(rows, s, r):
        return moved_columns_short(rows.reshape(size * rows_here, width), moves[s, r]).reshape(size, rows_here, width)

    with jax.named_scope("rows_first"):
        for q in range(chunks):
            part = slice(q * size, (q + 1) * size)
            row_state[part] = short_moved(stage[part], 0, 0)

    def first_step(rows):
        if groups > 1:
            tops[rows, :] = held[rows, :]
            return None
        moved = moved_columns(held[rows, :], moves[0, 0])
        state[rows, :] = moved
        return products([(moved, moved)])

    with jax.named_scope("a2a_wait"):
        held[rows_of(mine), :] = stage[mine]
        sums = first_step(rows_of(mine))
        for d in range(1, owners):
            incoming[d - 1].wait_recv()
            more = first_step(rows_of((mine + owners - d) % owners))
            if more is not None:
                sums = tuple(a + b for a, b in zip(sums, more))

    passing = []
    for s in range(steps):
        last = s + 1 == steps
        with jax.named_scope(f"solve{s}"):
            all_turns, told = solved(s, sums)
        if not last:
            with jax.named_scope(f"cross_send{s}"):
                parts = final_parts(s, all_turns)
                cut = rows_all // 2
                crossing = []
                for h in range(2):
                    bottoms[s, h] = parts[h][:, half:]
                    copy = pltpu.make_async_remote_copy(
                        bottoms.at[s, h], landed.at[s, h], mid_send.at[s, h], mid_recv.at[s, h],
                        device_id=(me, right), device_id_type=MESH)
                    copy.start()
                    crossing.append(copy)
                    tops[h * cut:(h + 1) * cut, :half] = parts[h][:, :half]
        if s > 0:
            with jax.named_scope(f"pass_wait{s}"):
                for copy in passing:
                    copy.wait()
            for q in range(chunks):
                part = slice(q * size, (q + 1) * size)
                rows = jnp.concatenate([row_tops[s - 1, part], row_landed[s - 1, part]], axis=2)
                row_state[part] = short_moved(rows, s, 0)
        passing = []
        for r in range(rounds):
            with jax.named_scope(f"told{s}_{r}"):
                for copy in told[r]:
                    copy.wait()
            with jax.named_scope(f"turn{s}_{r}"):
              for q in range(chunks):
                part = slice(q * size, (q + 1) * size)
                rows = rotated_columns(row_state[part], turns[s, r, part, 0:1, :], turns[s, r, part, 1:2, :])
                rows = short_moved(rows, s, r + 1)
                if r + 1 < rounds:
                    row_state[part] = rows
                    continue
                row_low[s, part] = rows[:, :, half:]
                copy = pltpu.make_async_remote_copy(
                    row_low.at[s, part], row_landed.at[s, part], row_send.at[s, q], row_recv.at[s, q],
                    device_id=(me, right), device_id_type=MESH)
                copy.start()
                passing.append(copy)
                if last:
                    for k in range(size):
                        out_ref[pl.ds(2 * (q * size + k), rows_here, stride=2 * owners), :] = rows[k, :, :half]
                else:
                    row_tops[s, part] = rows[:, :, :half]
        if not last:
            sums = None
            with jax.named_scope(f"cross_wait{s}"):
                for copy in crossing:
                    copy.wait()
            with jax.named_scope(f"cross_join{s}"):
                for h in range(2):
                    tops[h * cut:(h + 1) * cut, half:] = landed[s, h]
                if groups == 1:
                    parts = advanced(tops, None, s + 1, 0)
                    kept(state, parts)
                    sums = products([(part, part) for part in parts])

    for copy in incoming:
        copy.wait_send()
    for q in range(chunks):
        with jax.named_scope("last_pass"):
            passing[q].wait()
        for k in range(q * size, (q + 1) * size):
            out_ref[pl.ds(2 * k + 1, rows_here, stride=2 * owners), :] = row_landed[steps - 1, k]


def body(mesh_sizes, matrix, plan):
    rows_here, pair_here, halves, half = matrix.shape
    steps, rounds, width = plan.shape
    rows, cols = mesh_sizes
    owners, groups = pair_here, rows // pair_here
    assert rows % pair_here == 0 and halves == 2 and cols > 1
    sizes = (owners, groups, cols, rows_here, steps, rounds, width)
    dma = pltpu.SemaphoreType.DMA
    rows_all = owners * rows_here
    assert groups == 1 or rows_all >= 2 * width
    flat = (rows_here * pair_here * 2, half)
    anywhere = pl.BlockSpec(memory_space=pltpu.HBM)
    out = pl.pallas_call(
        functools.partial(kernel, sizes),
        out_shape=jax.ShapeDtypeStruct(flat, F32),
        in_specs=[anywhere, anywhere],
        out_specs=pl.BlockSpec(memory_space=pltpu.VMEM),
        scratch_shapes=[
            pltpu.VMEM(flat, F32),
            pltpu.VMEM((steps, rounds, width), jnp.int32),
            pltpu.VMEM((owners, rows_here, width), F32),
            pltpu.VMEM((rows_all, width), F32),
            pltpu.VMEM((rows_all if groups == 1 else 2 * width, width), F32),
            pltpu.VMEM((steps - 1, 2, rows_all // 2, half), F32),
            pltpu.VMEM((steps - 1, 2, rows_all // 2, half), F32),
            pltpu.VMEM((rows_all, width), F32),
            pltpu.VMEM((owners, rows_here, width), F32),
            pltpu.VMEM((steps - 1, owners, rows_here, half), F32),
            pltpu.VMEM((steps, owners, rows_here, half), F32),
            pltpu.VMEM((steps, owners, rows_here, half), F32),
            pltpu.VMEM((steps, rounds, owners, 2, half), F32),
            pltpu.VMEM((steps, rounds + 1, width, width), BF16),
            pltpu.VMEM((steps, rounds + 1, 8, width), jnp.int32),
            pltpu.VMEM((steps, groups, width, width) if groups > 1 else (1, 1, 8, 128), F32),
            dma((2,)), dma((owners,)), dma((owners,)), dma((steps, 2)), dma((steps, 2)),
            dma((steps, groups)), dma((steps, groups)),
            dma((steps, rounds, owners)), dma((steps, rounds, owners)), dma((steps, 2)), dma((steps, 2)),
        ],
        compiler_params=pltpu.CompilerParams(collective_id=0, has_side_effects=True, vmem_limit_bytes=40 << 20),
    )(matrix.reshape(flat), plan)
    return out.reshape(matrix.shape)


def solution(mesh):
    in_specs = (P("rows", "cols", None, None), P())
    out_specs = P("rows", "cols", None, None)
    sizes = (mesh.shape["rows"], mesh.shape["cols"])
    return jax.shard_map(functools.partial(body, sizes), mesh=mesh, in_specs=in_specs, out_specs=out_specs, check_vma=False)
```

```python
import functools

import jax
import jax.numpy as jnp
from jax import lax
from jax.experimental import pallas as pl
from jax.experimental.pallas import tpu as pltpu
from jax.sharding import PartitionSpec as P

MESH = pl.DeviceIdType.MESH
NN = (((1,), (0,)), ((), ()))
NT = (((1,), (1,)), ((), ()))
F32 = jnp.float32
BF16 = jnp.bfloat16


def dot(a, b, dims=NN, precision=None):
    return lax.dot_general(a, b, dims, precision=precision, preferred_element_type=F32)


def exact_dot(a, b, dims=NN):
    return dot(a, b, dims, lax.Precision.HIGHEST)


def moved_columns(a, onehot):
    hi = a.astype(BF16)
    rest = a - hi.astype(F32)
    mid = rest.astype(BF16)
    lo = (rest - mid.astype(F32)).astype(BF16)
    return dot(hi, onehot) + dot(mid, onehot) + dot(lo, onehot)


def moved_columns_short(a, onehot):
    hi = a.astype(BF16)
    mid = (a - hi.astype(F32)).astype(BF16)
    return dot(hi, onehot) + dot(mid, onehot)


def gathered_columns(a, source):
    rows, width = a.shape
    half = width // 2
    parts = []
    for h in range(2):
        index = source[:, h * half:(h + 1) * half]
        lane = jnp.broadcast_to(index % half, (rows, half))
        second = jnp.broadcast_to(index >= half, (rows, half))
        left, right = (
            jnp.take_along_axis(a[:, k * half:(k + 1) * half], lane, axis=1, mode="promise_in_bounds") for k in range(2))
        parts.append(jnp.where(second, right, left))
    return jnp.concatenate(parts, axis=1)


def rotated_columns(a, cosine, sine):
    half = a.shape[-1] // 2
    left, right = a[..., :half], a[..., half:]
    return jnp.concatenate([cosine * left - sine * right, sine * left + cosine * right], axis=-1)


def folded(a):
    return jnp.sum(a.reshape(-1, 8, a.shape[-1]), axis=0)


def products(factors):
    low = high = cross = 0.0
    for a, b in factors:
        half = a.shape[1] // 2
        low = low + folded(a[:, :half] * b[:, :half])
        high = high + folded(a[:, half:] * b[:, half:])
        cross = cross + folded(a[:, :half] * b[:, half:])
    return low, high, cross


def angles(sums):
    low, high, cross = (jnp.sum(v, axis=0, keepdims=True) for v in sums)
    spread = high - low
    sign = jnp.where(spread >= 0.0, 1.0, -1.0)
    root = jnp.sqrt(spread * spread + 4.0 * cross * cross)
    tangent = sign * 2.0 * cross / (jnp.abs(spread) + root)
    cosine = 1.0 / jnp.sqrt(1.0 + tangent * tangent)
    return cosine, tangent * cosine


def orders(partner):
    width = partner.shape[1]
    shape = (width, width)
    row = lax.broadcasted_iota(jnp.int32, shape, 0)
    col = lax.broadcasted_iota(jnp.int32, shape, 1)
    other = jnp.broadcast_to(partner, shape)
    swap = row == other
    one = jnp.ones(shape, BF16)

    def bits(mask):
        return jnp.where(mask, 1.0, 0.0).astype(BF16)

    swap_b = bits(swap)
    first_row = other > col
    rank_row = dot(bits(first_row), bits(row < col))
    mate_row = dot(rank_row.astype(BF16), swap_b)
    place_row = jnp.where(first_row, rank_row, mate_row + float(width // 2))
    first_col = dot(bits(swap & (col > row)), one) > 0.5
    rank_col = dot(bits(col < row), bits(first_col))
    mate_col = dot(swap_b, rank_col.astype(BF16))
    place_col = jnp.where(first_col, rank_col, mate_col + float(width // 2))
    forward = bits(place_col == col.astype(F32))
    backward = bits(place_row == row.astype(F32))
    return forward, backward


def kernel(sizes, x_hbm, plan_hbm, out_ref, x_ref, plan_ref, stage, held, state, bottoms, landed, tops, row_state,
           row_tops, row_low, row_landed, turns, moves, sources, grams, load_sem, in_send, in_recv, mid_send, mid_recv,
           gram_send, gram_recv, turn_send, turn_recv, row_send, row_recv):
    owners, groups, cols, rows_here, steps, rounds, width = sizes
    half = width // 2
    rows_all = owners * rows_here
    me = lax.axis_index("rows")
    col = lax.axis_index("cols")
    group, mine = me // owners, me % owners
    right = (col + 1) % cols

    def at(owner_shift, col_shift=0, group_shift=0):
        row = ((group + group_shift) % groups) * owners + (mine + owner_shift) % owners
        return row, (col + col_shift) % cols

    peers = {(o, 0, 0) for o in range(owners)} | {(0, c, 0) for c in (1, cols - 1)} | {(0, 0, g) for g in range(groups)}
    peers = sorted(peers - {(0, 0, 0)})
    barrier = pltpu.get_barrier_semaphore()
    for peer in peers:
        pl.semaphore_signal(barrier, inc=1, device_id=at(*peer), device_id_type=MESH)
    load = pltpu.make_async_copy(x_hbm, x_ref, load_sem.at[0])
    load.start()
    load_plan = pltpu.make_async_copy(plan_hbm, plan_ref, load_sem.at[1])
    load_plan.start()
    load.wait()
    for k in range(owners):
        for h in range(2):
            stage[k, :, h * half:(h + 1) * half] = x_ref[pl.ds(2 * k + h, rows_here, stride=2 * owners), :]
    with jax.named_scope("barrier_wait"):
        pl.semaphore_wait(barrier, len(peers))

    def rows_of(owner):
        return pl.ds(pl.multiple_of(owner * rows_here, rows_here), rows_here)

    incoming = []
    for d in range(1, owners):
        copy = pltpu.make_async_remote_copy(
            stage.at[(mine + d) % owners], held.at[rows_of(mine), :], in_send.at[0], in_recv.at[d],
            device_id=at(d), device_id_type=MESH)
        copy.start()
        incoming.append(copy)

    load_plan.wait()
    with jax.named_scope("orders"):
        ladder = lax.broadcasted_iota(jnp.int32, (8, width), 1).astype(F32).astype(BF16)
        for s in range(steps):
            before = None
            for r in range(rounds + 1):
                if r < rounds:
                    forward, backward = orders(plan_ref[s, r:r + 1, :])
                    move = forward if r == 0 else dot(before, forward).astype(BF16)
                    before = backward
                else:
                    move = before
                moves[s, r] = move
                sources[s, r] = dot(ladder, move).astype(jnp.int32)

    def advanced(ref, turn, s, r):
        parts = []
        cut = ref.shape[0] // 2
        for h in range(2):
            part = ref[h * cut:(h + 1) * cut, :]
            if turn is not None:
                part = rotated_columns(part, *turn)
            if h == 0:
                parts.append(moved_columns(part, moves[s, r]))
            else:
                parts.append(gathered_columns(part, sources[s, r, 0:1, :]))
        return parts

    def kept(ref, parts):
        cut = ref.shape[0] // 2
        for h in range(2):
            ref[h * cut:(h + 1) * cut, :] = parts[h]

    def tell(s, r, turn):
        cosine, sine = turn
        turns[s, r, mine] = jnp.concatenate([cosine, sine], axis=0)
        for d in range(1, owners):
            pltpu.make_async_remote_copy(
                turns.at[s, r, mine], turns.at[s, r, mine], turn_send.at[s], turn_recv.at[s, r],
                device_id=at(d), device_id_type=MESH).start()

    def all_told(s, r):
        block = turns.at[s, r, 0:owners - 1]
        return pltpu.make_async_remote_copy(
            block, block, turn_send.at[s], turn_recv.at[s, r], device_id=at(1), device_id_type=MESH)

    def all_tells(s):
        block = turns.at[s, :, 0:owners - 1]
        return pltpu.make_async_remote_copy(
            block, block, turn_send.at[s], turn_recv.at[s, 0], device_id=at(1), device_id_type=MESH)

    def solved(s, sums):
        if sums is None:
            x = tops[...]
            gram = exact_dot(x.T, x)
            grams[s, group] = gram
            shared = []
            for g in range(1, groups):
                copy = pltpu.make_async_remote_copy(
                    grams.at[s, group], grams.at[s, group], gram_send.at[s, g], gram_recv.at[s, g],
                    device_id=at(0, 0, g), device_id_type=MESH)
                copy.start()
                shared.append(copy)
            for copy in shared:
                copy.wait()
            gram = grams[s, 0]
            for g in range(1, groups):
                gram = gram + grams[s, g]
            state[0:width, :] = gram
            shape = (width, width)
            eye = lax.broadcasted_iota(jnp.int32, shape, 0) == lax.broadcasted_iota(jnp.int32, shape, 1)
            state[width:2 * width, :] = jnp.where(eye, 1.0, 0.0)
        turn, all_turns = None, []
        for r in range(rounds):
            if r > 0 or sums is None:
                parts = advanced(state, turn, s, r)
                kept(state, parts)
                factors = [tuple(parts)] if groups > 1 else [(part, part) for part in parts]
                sums = products(factors)
            turn = angles(sums)
            tell(s, r, turn)
            all_turns.append(turn)
        return all_turns

    def final_parts(s, all_turns):
        if groups > 1:
            turn = None
            for r in range(rounds):
                kept(tops, advanced(tops, turn, s, r))
                turn = all_turns[r]
            return advanced(tops, turn, s, rounds)
        return advanced(state, all_turns[-1], s, rounds)

    chunks = 2 if owners % 2 == 0 else 1
    size = owners // chunks

    def short_moved(q, rows, s, r):
        flat = rows.reshape(size * rows_here, width)
        if q % 2 == 0:
            flat = moved_columns_short(flat, moves[s, r])
        else:
            flat = gathered_columns(flat, sources[s, r, 0:1, :])
        return flat.reshape(size, rows_here, width)

    with jax.named_scope("rows_first"):
        for q in range(chunks):
            part = slice(q * size, (q + 1) * size)
            row_state[part] = short_moved(q, stage[part], 0, 0)

    def first_step(rows):
        if groups > 1:
            tops[rows, :] = held[rows, :]
            return None
        moved = moved_columns(held[rows, :], moves[0, 0])
        state[rows, :] = moved
        return products([(moved, moved)])

    with jax.named_scope("a2a_wait"):
        held[rows_of(mine), :] = stage[mine]
        sums = first_step(rows_of(mine))
        for d in range(1, owners):
            incoming[d - 1].wait_recv()
            more = first_step(rows_of((mine + owners - d) % owners))
            if more is not None:
                sums = tuple(a + b for a, b in zip(sums, more))

    passing = []
    for s in range(steps):
        last = s + 1 == steps
        with jax.named_scope(f"solve{s}"):
            all_turns = solved(s, sums)
        if not last:
            with jax.named_scope(f"cross_send{s}"):
                parts = final_parts(s, all_turns)
                cut = rows_all // 2
                crossing = []
                for h in range(2):
                    bottoms[s, h] = parts[h][:, half:]
                    copy = pltpu.make_async_remote_copy(
                        bottoms.at[s, h], landed.at[s, h], mid_send.at[s, h], mid_recv.at[s, h],
                        device_id=(me, right), device_id_type=MESH)
                    copy.start()
                    crossing.append(copy)
                    tops[h * cut:(h + 1) * cut, :half] = parts[h][:, :half]
        if s > 0:
            with jax.named_scope(f"pass_wait{s}"):
                for copy in passing:
                    copy.wait()
            for q in range(chunks):
                part = slice(q * size, (q + 1) * size)
                rows = jnp.concatenate([row_tops[s - 1, part], row_landed[s - 1, part]], axis=2)
                row_state[part] = short_moved(q, rows, s, 0)
        passing = []
        for r in range(rounds):
            with jax.named_scope(f"told{s}_{r}"):
                all_told(s, r).wait_recv()
            with jax.named_scope(f"turn{s}_{r}"):
                turned = []
                for q in range(chunks):
                    part = slice(q * size, (q + 1) * size)
                    rows = rotated_columns(row_state[part], turns[s, r, part, 0:1, :], turns[s, r, part, 1:2, :])
                    turned.append(short_moved(q, rows, s, r + 1))
                for q in range(chunks):
                    part = slice(q * size, (q + 1) * size)
                    if r + 1 < rounds:
                        row_state[part] = turned[q]
                        continue
                    row_low[s, part] = turned[q][:, :, half:]
                    copy = pltpu.make_async_remote_copy(
                        row_low.at[s, part], row_landed.at[s, part], row_send.at[s, q], row_recv.at[s, q],
                        device_id=(me, right), device_id_type=MESH)
                    copy.start()
                    passing.append(copy)
                    if last:
                        for k in range(size):
                            at_rows = pl.ds(2 * (q * size + k), rows_here, stride=2 * owners)
                            out_ref[at_rows, :] = turned[q][k, :, :half]
                    else:
                        row_tops[s, part] = turned[q][:, :, :half]
        if not last:
            sums = None
            with jax.named_scope(f"cross_wait{s}"):
                for copy in crossing:
                    copy.wait()
            with jax.named_scope(f"cross_join{s}"):
                for h in range(2):
                    tops[h * cut:(h + 1) * cut, half:] = landed[s, h]
                if groups == 1:
                    parts = advanced(tops, None, s + 1, 0)
                    kept(state, parts)
                    sums = products([(part, part) for part in parts])

    for s in range(steps):
        all_tells(s).wait_send()
    sent = stage.at[0:owners - 1]
    pltpu.make_async_remote_copy(sent, sent, in_send.at[0], in_recv.at[0], device_id=at(1), device_id_type=MESH).wait_send()
    for q in range(chunks):
        with jax.named_scope("last_pass"):
            passing[q].wait()
        for k in range(q * size, (q + 1) * size):
            out_ref[pl.ds(2 * k + 1, rows_here, stride=2 * owners), :] = row_landed[steps - 1, k]


def body(mesh_sizes, matrix, plan):
    rows_here, pair_here, halves, half = matrix.shape
    steps, rounds, width = plan.shape
    rows, cols = mesh_sizes
    owners, groups = pair_here, rows // pair_here
    assert rows % pair_here == 0 and halves == 2 and cols > 1
    sizes = (owners, groups, cols, rows_here, steps, rounds, width)
    dma = pltpu.SemaphoreType.DMA
    rows_all = owners * rows_here
    assert groups == 1 or rows_all >= 2 * width
    flat = (rows_here * pair_here * 2, half)
    anywhere = pl.BlockSpec(memory_space=pltpu.HBM)
    out = pl.pallas_call(
        functools.partial(kernel, sizes),
        out_shape=jax.ShapeDtypeStruct(flat, F32),
        in_specs=[anywhere, anywhere],
        out_specs=pl.BlockSpec(memory_space=pltpu.VMEM),
        scratch_shapes=[
            pltpu.VMEM(flat, F32),
            pltpu.VMEM((steps, rounds, width), jnp.int32),
            pltpu.VMEM((owners, rows_here, width), F32),
            pltpu.VMEM((rows_all, width), F32),
            pltpu.VMEM((rows_all if groups == 1 else 2 * width, width), F32),
            pltpu.VMEM((steps - 1, 2, rows_all // 2, half), F32),
            pltpu.VMEM((steps - 1, 2, rows_all // 2, half), F32),
            pltpu.VMEM((rows_all, width), F32),
            pltpu.VMEM((owners, rows_here, width), F32),
            pltpu.VMEM((steps - 1, owners, rows_here, half), F32),
            pltpu.VMEM((steps, owners, rows_here, half), F32),
            pltpu.VMEM((steps, owners, rows_here, half), F32),
            pltpu.VMEM((steps, rounds, owners, 2, half), F32),
            pltpu.VMEM((steps, rounds + 1, width, width), BF16),
            pltpu.VMEM((steps, rounds + 1, 8, width), jnp.int32),
            pltpu.VMEM((steps, groups, width, width) if groups > 1 else (1, 1, 8, 128), F32),
            dma((2,)), dma((1,)), dma((owners,)), dma((steps - 1, 2)), dma((steps - 1, 2)),
            dma((steps, groups) if groups > 1 else (1, 1)), dma((steps, groups) if groups > 1 else (1, 1)),
            dma((steps,)), dma((steps, rounds)), dma((steps, 2)), dma((steps, 2)),
        ],
        compiler_params=pltpu.CompilerParams(collective_id=0, has_side_effects=True, vmem_limit_bytes=40 << 20),
    )(pltpu.with_memory_space_constraint(matrix.reshape(flat), pltpu.HBM),
      pltpu.with_memory_space_constraint(plan, pltpu.HBM))
    return out.reshape(matrix.shape)


def solution(mesh):
    in_specs = (P("rows", "cols", None, None), P())
    out_specs = P("rows", "cols", None, None)
    sizes = (mesh.shape["rows"], mesh.shape["cols"])
    return jax.shard_map(functools.partial(body, sizes), mesh=mesh, in_specs=in_specs, out_specs=out_specs, check_vma=False)
```

```python
import functools

import jax
import jax.numpy as jnp
from jax import lax
from jax.experimental import pallas as pl
from jax.experimental.pallas import tpu as pltpu
from jax.sharding import PartitionSpec as P

MESH = pl.DeviceIdType.MESH
NN = (((1,), (0,)), ((), ()))
NT = (((1,), (1,)), ((), ()))
F32 = jnp.float32
BF16 = jnp.bfloat16


def dot(a, b, dims=NN, precision=None):
    return lax.dot_general(a, b, dims, precision=precision, preferred_element_type=F32)


def exact_dot(a, b, dims=NN):
    return dot(a, b, dims, lax.Precision.HIGHEST)


def moved_columns(a, onehot):
    hi = a.astype(BF16)
    rest = a - hi.astype(F32)
    mid = rest.astype(BF16)
    lo = (rest - mid.astype(F32)).astype(BF16)
    return dot(hi, onehot) + dot(mid, onehot) + dot(lo, onehot)


def moved_columns_short(a, onehot):
    hi = a.astype(BF16)
    mid = (a - hi.astype(F32)).astype(BF16)
    return dot(hi, onehot) + dot(mid, onehot)


def gathered_columns(a, source):
    rows, width = a.shape
    half = width // 2
    parts = []
    for h in range(2):
        index = source[:, h * half:(h + 1) * half]
        lane = jnp.broadcast_to(index % half, (rows, half))
        second = jnp.broadcast_to(index >= half, (rows, half))
        left, right = (
            jnp.take_along_axis(a[:, k * half:(k + 1) * half], lane, axis=1, mode="promise_in_bounds") for k in range(2))
        parts.append(jnp.where(second, right, left))
    return jnp.concatenate(parts, axis=1)


def rotated_columns(a, cosine, sine):
    half = a.shape[-1] // 2
    left, right = a[..., :half], a[..., half:]
    return jnp.concatenate([cosine * left - sine * right, sine * left + cosine * right], axis=-1)


def folded(a):
    return jnp.sum(a.reshape(-1, 8, a.shape[-1]), axis=0)


def products(factors):
    low = high = cross = 0.0
    for a, b in factors:
        half = a.shape[1] // 2
        low = low + folded(a[:, :half] * b[:, :half])
        high = high + folded(a[:, half:] * b[:, half:])
        cross = cross + folded(a[:, :half] * b[:, half:])
    return low, high, cross


def angles(sums):
    low, high, cross = (jnp.sum(v, axis=0, keepdims=True) for v in sums)
    spread = high - low
    sign = jnp.where(spread >= 0.0, 1.0, -1.0)
    root = jnp.sqrt(spread * spread + 4.0 * cross * cross)
    tangent = sign * 2.0 * cross / (jnp.abs(spread) + root)
    cosine = lax.rsqrt(1.0 + tangent * tangent)
    return cosine, tangent * cosine


def orders(partner):
    width = partner.shape[1]
    shape = (width, width)
    row = lax.broadcasted_iota(jnp.int32, shape, 0)
    col = lax.broadcasted_iota(jnp.int32, shape, 1)
    other = jnp.broadcast_to(partner, shape)
    swap = row == other
    one = jnp.ones(shape, BF16)

    def bits(mask):
        return jnp.where(mask, 1.0, 0.0).astype(BF16)

    swap_b = bits(swap)
    first_row = other > col
    rank_row = dot(bits(first_row), bits(row < col))
    mate_row = dot(rank_row.astype(BF16), swap_b)
    place_row = jnp.where(first_row, rank_row, mate_row + float(width // 2))
    first_col = dot(bits(swap & (col > row)), one) > 0.5
    rank_col = dot(bits(col < row), bits(first_col))
    mate_col = dot(swap_b, rank_col.astype(BF16))
    place_col = jnp.where(first_col, rank_col, mate_col + float(width // 2))
    forward = bits(place_col == col.astype(F32))
    backward = bits(place_row == row.astype(F32))
    return forward, backward


def kernel(sizes, x_hbm, plan_hbm, out_ref, x_ref, plan_ref, stage, held, state, bottoms, landed, tops, row_state,
           row_tops, row_low, row_landed, finals, turns, moves, sources, grams, load_sem, in_send, in_recv, mid_send, mid_recv,
           gram_send, gram_recv, turn_send, turn_recv, row_send, row_recv, direct):
    owners, groups, cols, rows_here, steps, rounds, width = sizes
    half = width // 2
    rows_all = owners * rows_here
    me = lax.axis_index("rows")
    col = lax.axis_index("cols")
    group, mine = me // owners, me % owners
    right = (col + 1) % cols

    def at(owner_shift, col_shift=0, group_shift=0):
        row = ((group + group_shift) % groups) * owners + (mine + owner_shift) % owners
        return row, (col + col_shift) % cols

    peers = {(o, 0, 0) for o in range(owners)} | {(0, c, 0) for c in (1, cols - 1)} | {(0, 0, g) for g in range(groups)}
    peers = sorted(peers - {(0, 0, 0)})
    barrier = pltpu.get_barrier_semaphore()
    for peer in peers:
        pl.semaphore_signal(barrier, inc=1, device_id=at(*peer), device_id_type=MESH)
    load = pltpu.make_async_copy(x_hbm, x_ref, load_sem.at[0])
    load.start()
    load_plan = pltpu.make_async_copy(plan_hbm, plan_ref, load_sem.at[1])
    load_plan.start()
    load.wait()
    for k in range(owners):
        for h in range(2):
            stage[k, :, h * half:(h + 1) * half] = x_ref[pl.ds(2 * k + h, rows_here, stride=2 * owners), :]
    with jax.named_scope("barrier_wait"):
        pl.semaphore_wait(barrier, len(peers))

    def rows_of(owner):
        return pl.ds(pl.multiple_of(owner * rows_here, rows_here), rows_here)

    incoming = []
    for d in range(1, owners):
        copy = pltpu.make_async_remote_copy(
            stage.at[(mine + d) % owners], held.at[rows_of(mine), :], in_send.at[0], in_recv.at[d],
            device_id=at(d), device_id_type=MESH)
        copy.start()
        incoming.append(copy)

    load_plan.wait()
    with jax.named_scope("orders"):
        ladder = lax.broadcasted_iota(jnp.int32, (8, width), 1).astype(F32).astype(BF16)
        for s in range(steps):
            before = None
            for r in range(rounds + 1):
                if r < rounds:
                    forward, backward = orders(plan_ref[s, r:r + 1, :])
                    move = forward if r == 0 else dot(before, forward).astype(BF16)
                    before = backward
                else:
                    move = before
                moves[s, r] = move
                sources[s, r] = dot(ladder, move).astype(jnp.int32)

    def advanced(ref, turn, s, r):
        parts = []
        cut = ref.shape[0] // 2
        for h in range(2):
            part = ref[h * cut:(h + 1) * cut, :]
            if turn is not None:
                part = rotated_columns(part, *turn)
            if h == 0:
                parts.append(moved_columns(part, moves[s, r]))
            else:
                parts.append(gathered_columns(part, sources[s, r, 0:1, :]))
        return parts

    def kept(ref, parts):
        cut = ref.shape[0] // 2
        for h in range(2):
            ref[h * cut:(h + 1) * cut, :] = parts[h]

    def tell(s, r, turn):
        cosine, sine = turn
        turns[s, r, mine] = jnp.concatenate([cosine, sine], axis=0)
        for d in range(1, owners):
            pltpu.make_async_remote_copy(
                turns.at[s, r, mine], turns.at[s, r, mine], turn_send.at[s], turn_recv.at[s, r],
                device_id=at(d), device_id_type=MESH).start()

    def all_told(s, r):
        block = turns.at[s, r, 0:owners - 1]
        return pltpu.make_async_remote_copy(
            block, block, turn_send.at[s], turn_recv.at[s, r], device_id=at(1), device_id_type=MESH)

    def all_tells(s):
        block = turns.at[s, :, 0:owners - 1]
        return pltpu.make_async_remote_copy(
            block, block, turn_send.at[s], turn_recv.at[s, 0], device_id=at(1), device_id_type=MESH)

    def solved(s, sums):
        if sums is None:
            x = tops[...]
            gram = exact_dot(x.T, x)
            grams[s, group] = gram
            shared = []
            for g in range(1, groups):
                copy = pltpu.make_async_remote_copy(
                    grams.at[s, group], grams.at[s, group], gram_send.at[s, g], gram_recv.at[s, g],
                    device_id=at(0, 0, g), device_id_type=MESH)
                copy.start()
                shared.append(copy)
            for copy in shared:
                copy.wait()
            gram = grams[s, 0]
            for g in range(1, groups):
                gram = gram + grams[s, g]
            state[0:width, :] = gram
            shape = (width, width)
            eye = lax.broadcasted_iota(jnp.int32, shape, 0) == lax.broadcasted_iota(jnp.int32, shape, 1)
            state[width:2 * width, :] = jnp.where(eye, 1.0, 0.0)
        turn, all_turns = None, []
        for r in range(rounds):
            if r > 0 or sums is None:
                parts = advanced(state, turn, s, r)
                kept(state, parts)
                factors = [tuple(parts)] if groups > 1 else [(part, part) for part in parts]
                sums = products(factors)
            turn = angles(sums)
            tell(s, r, turn)
            all_turns.append(turn)
        return all_turns

    def final_parts(s, all_turns):
        if groups > 1:
            turn = None
            for r in range(rounds):
                kept(tops, advanced(tops, turn, s, r))
                turn = all_turns[r]
            return advanced(tops, turn, s, rounds)
        return advanced(state, all_turns[-1], s, rounds)

    chunks = 2
    size = owners // chunks
    side = mine // size

    def short_moved(q, rows, s, r):
        flat = rows.reshape(size * rows_here, width)
        if q % 2 == 0:
            flat = moved_columns_short(flat, moves[s, r])
        else:
            flat = gathered_columns(flat, sources[s, r, 0:1, :])
        return flat.reshape(size, rows_here, width)

    with jax.named_scope("rows_first"):
        for q in range(chunks):
            part = slice(q * size, (q + 1) * size)
            row_state[part] = short_moved(q, stage[part], 0, 0)

    def first_step(rows):
        if groups > 1:
            tops[rows, :] = held[rows, :]
            return None
        moved = moved_columns(held[rows, :], moves[0, 0])
        state[rows, :] = moved
        return products([(moved, moved)])

    with jax.named_scope("a2a_wait"):
        held[rows_of(mine), :] = stage[mine]
        sums = first_step(rows_of(mine))
        for d in range(1, owners):
            incoming[d - 1].wait_recv()
            more = first_step(rows_of((mine + owners - d) % owners))
            if more is not None:
                sums = tuple(a + b for a, b in zip(sums, more))

    passing = []
    for s in range(steps):
        last = s + 1 == steps
        with jax.named_scope(f"solve{s}"):
            all_turns = solved(s, sums)
        if not last:
            with jax.named_scope(f"cross_send{s}"):
                parts = final_parts(s, all_turns)
                cut = rows_all // 2
                crossing = []
                for h in range(2):
                    bottoms[s, h] = parts[h][:, half:]
                    copy = pltpu.make_async_remote_copy(
                        bottoms.at[s, h], landed.at[s, h], mid_send.at[s, h], mid_recv.at[s, h],
                        device_id=(me, right), device_id_type=MESH)
                    copy.start()
                    crossing.append(copy)
                    tops[h * cut:(h + 1) * cut, :half] = parts[h][:, :half]
        else:
            with jax.named_scope("direct_send"):
                parts = final_parts(s, all_turns)
                cut = rows_all // 2
                for h in range(2):
                    finals[h * cut:(h + 1) * cut, :] = parts[h][:, half:]
                for j in range(size):
                    owner = side * size + (mine + j) % size
                    pltpu.make_async_remote_copy(
                        finals.at[rows_of(owner), :], row_landed.at[s, mine], direct.at[0], direct.at[1],
                        device_id=(group * owners + owner, right), device_id_type=MESH).start()
        if s > 0:
            with jax.named_scope(f"pass_wait{s}"):
                for copy in passing:
                    copy.wait()
            for q in range(chunks):
                part = slice(q * size, (q + 1) * size)
                rows = jnp.concatenate([row_tops[s - 1, part], row_landed[s - 1, part]], axis=2)
                row_state[part] = short_moved(q, rows, s, 0)
        passing = []
        for r in range(rounds):
            with jax.named_scope(f"told{s}_{r}"):
                all_told(s, r).wait_recv()
            with jax.named_scope(f"turn{s}_{r}"):
                turned = []
                for q in range(chunks):
                    part = slice(q * size, (q + 1) * size)
                    rows = rotated_columns(row_state[part], turns[s, r, part, 0:1, :], turns[s, r, part, 1:2, :])
                    turned.append(short_moved(q, rows, s, r + 1))
                for q in range(chunks):
                    part = slice(q * size, (q + 1) * size)
                    if r + 1 < rounds:
                        row_state[part] = turned[q]
                        continue
                    row_low[s, part] = turned[q][:, :, half:]
                    slot = 0 if last else q
                    copy = pltpu.make_async_remote_copy(
                        row_low.at[s, part], row_landed.at[s, part], row_send.at[s, slot], row_recv.at[s, slot],
                        device_id=(me, right), device_id_type=MESH)
                    if last:
                        pl.when(side != q)(copy.start)
                    else:
                        copy.start()
                    passing.append(copy)
                    if last:
                        for k in range(size):
                            at_rows = pl.ds(2 * (q * size + k), rows_here, stride=2 * owners)
                            out_ref[at_rows, :] = turned[q][k, :, :half]
                    else:
                        row_tops[s, part] = turned[q][:, :, :half]
        if not last:
            sums = None
            with jax.named_scope(f"cross_wait{s}"):
                for copy in crossing:
                    copy.wait()
            with jax.named_scope(f"cross_join{s}"):
                for h in range(2):
                    tops[h * cut:(h + 1) * cut, half:] = landed[s, h]
                if groups == 1:
                    parts = advanced(tops, None, s + 1, 0)
                    kept(state, parts)
                    sums = products([(part, part) for part in parts])

    for s in range(steps):
        all_tells(s).wait_send()
    sent = stage.at[0:owners - 1]
    pltpu.make_async_remote_copy(sent, sent, in_send.at[0], in_recv.at[0], device_id=at(1), device_id_type=MESH).wait_send()
    def put_bottoms(q):
        for k in range(q * size, (q + 1) * size):
            out_ref[pl.ds(2 * k + 1, rows_here, stride=2 * owners), :] = row_landed[steps - 1, k]

    near = row_landed.at[steps - 1, 0:size]
    with jax.named_scope("direct_wait"):
        pltpu.make_async_remote_copy(
            near, near, direct.at[0], direct.at[1], device_id=(me, right), device_id_type=MESH).wait()
    for q in range(chunks):
        pl.when(side == q)(functools.partial(put_bottoms, q))
    with jax.named_scope("last_pass"):
        passing[0].wait()
    for q in range(chunks):
        pl.when(side != q)(functools.partial(put_bottoms, q))


def body(mesh_sizes, matrix, plan):
    rows_here, pair_here, halves, half = matrix.shape
    steps, rounds, width = plan.shape
    rows, cols = mesh_sizes
    owners, groups = pair_here, rows // pair_here
    assert rows % pair_here == 0 and pair_here % 2 == 0 and halves == 2 and cols > 1
    sizes = (owners, groups, cols, rows_here, steps, rounds, width)
    dma = pltpu.SemaphoreType.DMA
    rows_all = owners * rows_here
    assert groups == 1 or rows_all >= 2 * width
    flat = (rows_here * pair_here * 2, half)
    anywhere = pl.BlockSpec(memory_space=pltpu.HBM)
    out = pl.pallas_call(
        functools.partial(kernel, sizes),
        out_shape=jax.ShapeDtypeStruct(flat, F32),
        in_specs=[anywhere, anywhere],
        out_specs=pl.BlockSpec(memory_space=pltpu.VMEM),
        scratch_shapes=[
            pltpu.VMEM(flat, F32),
            pltpu.VMEM((steps, rounds, width), jnp.int32),
            pltpu.VMEM((owners, rows_here, width), F32),
            pltpu.VMEM((rows_all, width), F32),
            pltpu.VMEM((rows_all if groups == 1 else 2 * width, width), F32),
            pltpu.VMEM((steps - 1, 2, rows_all // 2, half), F32),
            pltpu.VMEM((steps - 1, 2, rows_all // 2, half), F32),
            pltpu.VMEM((rows_all, width), F32),
            pltpu.VMEM((owners, rows_here, width), F32),
            pltpu.VMEM((steps - 1, owners, rows_here, half), F32),
            pltpu.VMEM((steps, owners, rows_here, half), F32),
            pltpu.VMEM((steps, owners, rows_here, half), F32),
            pltpu.VMEM((rows_all, half), F32),
            pltpu.VMEM((steps, rounds, owners, 2, half), F32),
            pltpu.VMEM((steps, rounds + 1, width, width), BF16),
            pltpu.VMEM((steps, rounds + 1, 8, width), jnp.int32),
            pltpu.VMEM((steps, groups, width, width) if groups > 1 else (1, 1, 8, 128), F32),
            dma((2,)), dma((1,)), dma((owners,)), dma((steps - 1, 2)), dma((steps - 1, 2)),
            dma((steps, groups) if groups > 1 else (1, 1)), dma((steps, groups) if groups > 1 else (1, 1)),
            dma((steps,)), dma((steps, rounds)), dma((steps, 2)), dma((steps, 2)), dma((2,)),
        ],
        compiler_params=pltpu.CompilerParams(collective_id=0, has_side_effects=True, vmem_limit_bytes=40 << 20),
    )(pltpu.with_memory_space_constraint(matrix.reshape(flat), pltpu.HBM),
      pltpu.with_memory_space_constraint(plan, pltpu.HBM))
    return out.reshape(matrix.shape)


def solution(mesh):
    in_specs = (P("rows", "cols", None, None), P())
    out_specs = P("rows", "cols", None, None)
    sizes = (mesh.shape["rows"], mesh.shape["cols"])
    return jax.shard_map(functools.partial(body, sizes), mesh=mesh, in_specs=in_specs, out_specs=out_specs, check_vma=False)
```

```python
import functools

import jax
import jax.numpy as jnp
from jax import lax
from jax.experimental import pallas as pl
from jax.experimental.pallas import tpu as pltpu
from jax.sharding import PartitionSpec as P

MESH = pl.DeviceIdType.MESH
NN = (((1,), (0,)), ((), ()))
NT = (((1,), (1,)), ((), ()))
F32 = jnp.float32
BF16 = jnp.bfloat16


def dot(a, b, dims=NN, precision=None):
    return lax.dot_general(a, b, dims, precision=precision, preferred_element_type=F32)


def exact_dot(a, b, dims=NN):
    return dot(a, b, dims, lax.Precision.HIGHEST)


def moved_columns(a, onehot):
    hi = a.astype(BF16)
    rest = a - hi.astype(F32)
    mid = rest.astype(BF16)
    lo = (rest - mid.astype(F32)).astype(BF16)
    return dot(hi, onehot) + dot(mid, onehot) + dot(lo, onehot)


def moved_columns_short(a, onehot):
    hi = a.astype(BF16)
    mid = (a - hi.astype(F32)).astype(BF16)
    return dot(hi, onehot) + dot(mid, onehot)


def gathered_columns(a, source):
    rows, width = a.shape
    half = width // 2
    parts = []
    for h in range(2):
        index = source[:, h * half:(h + 1) * half]
        lane = jnp.broadcast_to(index % half, (rows, half))
        second = jnp.broadcast_to(index >= half, (rows, half))
        left, right = (
            jnp.take_along_axis(a[:, k * half:(k + 1) * half], lane, axis=1, mode="promise_in_bounds") for k in range(2))
        parts.append(jnp.where(second, right, left))
    return jnp.concatenate(parts, axis=1)


def rotated_columns(a, cosine, sine):
    half = a.shape[-1] // 2
    left, right = a[..., :half], a[..., half:]
    return jnp.concatenate([cosine * left - sine * right, sine * left + cosine * right], axis=-1)


def folded(a):
    return jnp.sum(a.reshape(-1, 8, a.shape[-1]), axis=0)


def products(factors):
    low = high = cross = 0.0
    for a, b in factors:
        half = a.shape[1] // 2
        low = low + folded(a[:, :half] * b[:, :half])
        high = high + folded(a[:, half:] * b[:, half:])
        cross = cross + folded(a[:, :half] * b[:, half:])
    return low, high, cross


def angles(sums):
    low, high, cross = (jnp.sum(v, axis=0, keepdims=True) for v in sums)
    spread = high - low
    sign = jnp.where(spread >= 0.0, 1.0, -1.0)
    root = jnp.sqrt(spread * spread + 4.0 * cross * cross)
    tangent = sign * 2.0 * cross / (jnp.abs(spread) + root)
    cosine = lax.rsqrt(1.0 + tangent * tangent)
    return cosine, tangent * cosine


def orders(partner):
    width = partner.shape[1]
    shape = (width, width)
    row = lax.broadcasted_iota(jnp.int32, shape, 0)
    col = lax.broadcasted_iota(jnp.int32, shape, 1)
    other = jnp.broadcast_to(partner, shape)
    swap = row == other
    one = jnp.ones(shape, BF16)

    def bits(mask):
        return jnp.where(mask, 1.0, 0.0).astype(BF16)

    swap_b = bits(swap)
    first_row = other > col
    rank_row = dot(bits(first_row), bits(row < col))
    mate_row = dot(rank_row.astype(BF16), swap_b)
    place_row = jnp.where(first_row, rank_row, mate_row + float(width // 2))
    first_col = dot(bits(swap & (col > row)), one) > 0.5
    rank_col = dot(bits(col < row), bits(first_col))
    mate_col = dot(swap_b, rank_col.astype(BF16))
    place_col = jnp.where(first_col, rank_col, mate_col + float(width // 2))
    forward = bits(place_col == col.astype(F32))
    backward = bits(place_row == row.astype(F32))
    return forward, backward


def kernel(sizes, x_hbm, plan_hbm, out_ref, x_ref, plan_ref, stage, held, state, bottoms, landed, tops, row_state,
           row_tops, row_low, row_landed, turns, moves, sources, grams, clear, load_sem, in_send, in_recv, mid_send, mid_recv,
           gram_send, gram_recv, turn_send, turn_recv, row_send, row_recv, direct):
    owners, groups, cols, rows_here, steps, rounds, width = sizes
    half = width // 2
    rows_all = owners * rows_here
    me = lax.axis_index("rows")
    col = lax.axis_index("cols")
    group, mine = me // owners, me % owners
    right = (col + 1) % cols

    def at(owner_shift, col_shift=0, group_shift=0):
        row = ((group + group_shift) % groups) * owners + (mine + owner_shift) % owners
        return row, (col + col_shift) % cols

    peers = {(o, 0, 0) for o in range(owners)} | {(0, c, 0) for c in (1, cols - 1)} | {(0, 0, g) for g in range(groups)}
    peers = sorted(peers - {(0, 0, 0)})
    barrier = pltpu.get_barrier_semaphore()
    for peer in peers:
        pl.semaphore_signal(barrier, inc=1, device_id=at(*peer), device_id_type=MESH)
    load = pltpu.make_async_copy(x_hbm, x_ref, load_sem.at[0])
    load.start()
    load_plan = pltpu.make_async_copy(plan_hbm, plan_ref, load_sem.at[1])
    load_plan.start()
    load.wait()
    for k in range(owners):
        for h in range(2):
            stage[k, :, h * half:(h + 1) * half] = x_ref[pl.ds(2 * k + h, rows_here, stride=2 * owners), :]
    with jax.named_scope("barrier_wait"):
        pl.semaphore_wait(barrier, len(peers))

    def rows_of(owner):
        return pl.ds(pl.multiple_of(owner * rows_here, rows_here), rows_here)

    incoming = {}
    order = sorted(range(1, owners), key=lambda d: (abs(d - owners // 2), d))
    first = owners - 6
    for i, d in enumerate(order):
        incoming[d] = pltpu.make_async_remote_copy(
            stage.at[(mine + d) % owners], held.at[rows_of(mine), :], in_send.at[int(i + 1 >= first)], in_recv.at[d],
            device_id=at(d), device_id_type=MESH)

    def send_rows():
        for d in order:
            incoming[d].start()

    def rows_sent(slot, count):
        sent = stage.at[0:count]
        pltpu.make_async_remote_copy(
            sent, sent, in_send.at[slot], in_recv.at[0], device_id=at(1), device_id_type=MESH).wait_send()

    early = col % 2 == 1
    pl.when(early)(send_rows)
    load_plan.wait()
    ladder = lax.broadcasted_iota(jnp.int32, (8, width), 1).astype(F32).astype(BF16)

    def arrange(s):
        before = None
        for r in range(rounds + 1):
            if r < rounds:
                forward, backward = orders(plan_ref[s, r:r + 1, :])
                move = forward if r == 0 else dot(before, forward).astype(BF16)
                before = backward
            else:
                move = before
            moves[s, r] = move
            sources[s, r] = dot(ladder, move).astype(jnp.int32)

    with jax.named_scope("orders0"):
        arrange(0)

    with jax.named_scope("hand_over"):
        @pl.when(early)
        def _():
            rows_sent(0, first - 1)
            partner = (me, (col + cols - 1) % cols)
            pl.semaphore_signal(clear.at[0], inc=1, device_id=partner, device_id_type=MESH)

        @pl.when(jnp.logical_not(early))
        def _():
            pl.semaphore_wait(clear.at[0], 1)
            send_rows()

    with jax.named_scope("orders1"):
        for s in range(1, steps):
            arrange(s)

    def advanced(ref, turn, s, r):
        parts = []
        cut = ref.shape[0] // 2
        for h in range(2):
            part = ref[h * cut:(h + 1) * cut, :]
            if turn is not None:
                part = rotated_columns(part, *turn)
            if h == 0:
                parts.append(moved_columns(part, moves[s, r]))
            else:
                parts.append(gathered_columns(part, sources[s, r, 0:1, :]))
        return parts

    def kept(ref, parts):
        cut = ref.shape[0] // 2
        for h in range(2):
            ref[h * cut:(h + 1) * cut, :] = parts[h]

    def tell(s, r, turn):
        cosine, sine = turn
        turns[s, r, mine] = jnp.concatenate([cosine, sine], axis=0)
        for d in range(1, owners):
            pltpu.make_async_remote_copy(
                turns.at[s, r, mine], turns.at[s, r, mine], turn_send.at[s], turn_recv.at[s, r],
                device_id=at(d), device_id_type=MESH).start()

    def all_told(s, r):
        block = turns.at[s, r, 0:owners - 1]
        return pltpu.make_async_remote_copy(
            block, block, turn_send.at[s], turn_recv.at[s, r], device_id=at(1), device_id_type=MESH)

    def all_tells(s):
        block = turns.at[s, :, 0:owners - 1]
        return pltpu.make_async_remote_copy(
            block, block, turn_send.at[s], turn_recv.at[s, 0], device_id=at(1), device_id_type=MESH)

    def solved(s, sums):
        if sums is None:
            x = tops[...]
            gram = exact_dot(x.T, x)
            grams[s, group] = gram
            shared = []
            for g in range(1, groups):
                copy = pltpu.make_async_remote_copy(
                    grams.at[s, group], grams.at[s, group], gram_send.at[s, g], gram_recv.at[s, g],
                    device_id=at(0, 0, g), device_id_type=MESH)
                copy.start()
                shared.append(copy)
            for copy in shared:
                copy.wait()
            gram = grams[s, 0]
            for g in range(1, groups):
                gram = gram + grams[s, g]
            state[0:width, :] = gram
            shape = (width, width)
            eye = lax.broadcasted_iota(jnp.int32, shape, 0) == lax.broadcasted_iota(jnp.int32, shape, 1)
            state[width:2 * width, :] = jnp.where(eye, 1.0, 0.0)
        turn, all_turns = None, []
        for r in range(rounds):
            if r > 0 or sums is None:
                parts = advanced(state, turn, s, r)
                kept(state, parts)
                factors = [tuple(parts)] if groups > 1 else [(part, part) for part in parts]
                sums = products(factors)
            turn = angles(sums)
            tell(s, r, turn)
            all_turns.append(turn)
        return all_turns

    def final_parts(s, all_turns):
        if groups > 1:
            turn = None
            for r in range(rounds):
                kept(tops, advanced(tops, turn, s, r))
                turn = all_turns[r]
            return advanced(tops, turn, s, rounds)
        return advanced(state, all_turns[-1], s, rounds)

    chunks = 2
    size = owners // chunks
    side = mine // size

    def near_landed(s, count):
        block = row_landed.at[s, 0:count]
        return pltpu.make_async_remote_copy(
            block, block, direct.at[0, s], direct.at[1, s], device_id=(me, right), device_id_type=MESH)

    def short_moved(q, rows, s, r):
        flat = rows.reshape(size * rows_here, width)
        if q % 2 == 0:
            flat = moved_columns_short(flat, moves[s, r])
        else:
            flat = gathered_columns(flat, sources[s, r, 0:1, :])
        return flat.reshape(size, rows_here, width)

    with jax.named_scope("rows_first"):
        for q in range(chunks):
            part = slice(q * size, (q + 1) * size)
            row_state[part] = short_moved(q, stage[part], 0, 0)

    def first_step(rows):
        if groups > 1:
            tops[rows, :] = held[rows, :]
            return None
        moved = moved_columns(held[rows, :], moves[0, 0])
        state[rows, :] = moved
        return products([(moved, moved)])

    with jax.named_scope("a2a_wait"):
        held[rows_of(mine), :] = stage[mine]
        sums = first_step(rows_of(mine))
        for d in reversed(order):
            incoming[d].wait_recv()
            more = first_step(rows_of((mine + owners - d) % owners))
            if more is not None:
                sums = tuple(a + b for a, b in zip(sums, more))

    cut = rows_all // 2

    def crossing(s, h):
        return pltpu.make_async_remote_copy(
            bottoms.at[s, h], landed.at[s, h], mid_send.at[s, h], mid_recv.at[s, h],
            device_id=(me, right), device_id_type=MESH)

    def passing(s, q=0):
        part = slice(q * size, (q + 1) * size)
        return pltpu.make_async_remote_copy(
            row_low.at[s, part], row_landed.at[s, part], row_send.at[s], row_recv.at[s],
            device_id=(me, right), device_id_type=MESH)

    def solve(s, sums):
        last = s + 1 == steps
        with jax.named_scope(f"solve{s}"):
            all_turns = solved(s, sums)
        with jax.named_scope(f"send{s}"):
            parts = final_parts(s, all_turns)
            for h in range(2):
                bottoms[s, h] = parts[h][:, half:]
                if last:
                    continue
                crossing(s, h).start()
                tops[h * cut:(h + 1) * cut, :half] = parts[h][:, :half]
            for j in range(0 if last else 1, size):
                other = (mine + j) % size
                pltpu.make_async_remote_copy(
                    bottoms.at[s, side, rows_of(other), :], row_landed.at[s, mine], direct.at[0, s], direct.at[1, s],
                    device_id=(group * owners + side * size + other, right), device_id_type=MESH).start()

    def rows_step(s):
        last = s + 1 == steps
        if s > 0:
            with jax.named_scope(f"pass_wait{s}"):
                near_landed(s - 1, size - 1).wait()
                passing(s - 1).wait()
            for q in range(chunks):
                part = slice(q * size, (q + 1) * size)
                rows = jnp.concatenate([row_tops[s - 1, part], row_landed[s - 1, part]], axis=2)
                row_state[part] = short_moved(q, rows, s, 0)
        for r in range(rounds):
            with jax.named_scope(f"told{s}_{r}"):
                all_told(s, r).wait_recv()
            with jax.named_scope(f"turn{s}_{r}"):
                turned = []
                for q in range(chunks):
                    part = slice(q * size, (q + 1) * size)
                    rows = rotated_columns(row_state[part], turns[s, r, part, 0:1, :], turns[s, r, part, 1:2, :])
                    turned.append(short_moved(q, rows, s, r + 1))
                for q in range(chunks):
                    part = slice(q * size, (q + 1) * size)
                    if r + 1 < rounds:
                        row_state[part] = turned[q]
                        continue
                    row_low[s, part] = turned[q][:, :, half:]
                    pl.when(side != q)(passing(s, q).start)
                    if last:
                        for k in range(size):
                            at_rows = pl.ds(2 * (q * size + k), rows_here, stride=2 * owners)
                            out_ref[at_rows, :] = turned[q][k, :, :half]
                    else:
                        row_tops[s, part] = turned[q][:, :, :half]

    def join(s):
        with jax.named_scope(f"cross_wait{s}"):
            for h in range(2):
                crossing(s, h).wait()
        with jax.named_scope(f"cross_join{s}"):
            for h in range(2):
                tops[h * cut:(h + 1) * cut, half:] = landed[s, h]
            row_landed[s, mine] = landed[s, side, rows_of(mine % size), :]
            if groups > 1:
                return None
            parts = advanced(tops, None, s + 1, 0)
            kept(state, parts)
            return products([(part, part) for part in parts])

    solve(0, sums)
    ahead = col % 2 == 0
    for s in range(steps - 1):
        @pl.when(ahead)
        def _():
            solve(s + 1, join(s))
            rows_step(s)

        @pl.when(jnp.logical_not(ahead))
        def _():
            rows_step(s)
            solve(s + 1, join(s))

    rows_step(steps - 1)

    for s in range(steps):
        all_tells(s).wait_send()
    pl.when(jnp.logical_not(early))(functools.partial(rows_sent, 0, first - 1))
    rows_sent(1, owners - first)

    def put_bottoms(q):
        for k in range(q * size, (q + 1) * size):
            out_ref[pl.ds(2 * k + 1, rows_here, stride=2 * owners), :] = row_landed[steps - 1, k]

    with jax.named_scope("direct_wait"):
        near_landed(steps - 1, size).wait()
    for q in range(chunks):
        pl.when(side == q)(functools.partial(put_bottoms, q))
    with jax.named_scope("last_pass"):
        passing(steps - 1).wait()
    for q in range(chunks):
        pl.when(side != q)(functools.partial(put_bottoms, q))


def body(mesh_sizes, matrix, plan):
    rows_here, pair_here, halves, half = matrix.shape
    steps, rounds, width = plan.shape
    rows, cols = mesh_sizes
    owners, groups = pair_here, rows // pair_here
    assert rows % pair_here == 0 and pair_here % 2 == 0 and halves == 2 and cols > 1 and cols % 2 == 0
    sizes = (owners, groups, cols, rows_here, steps, rounds, width)
    dma = pltpu.SemaphoreType.DMA
    rows_all = owners * rows_here
    assert groups == 1 or rows_all >= 2 * width
    flat = (rows_here * pair_here * 2, half)
    anywhere = pl.BlockSpec(memory_space=pltpu.HBM)
    out = pl.pallas_call(
        functools.partial(kernel, sizes),
        out_shape=jax.ShapeDtypeStruct(flat, F32),
        in_specs=[anywhere, anywhere],
        out_specs=pl.BlockSpec(memory_space=pltpu.VMEM),
        scratch_shapes=[
            pltpu.VMEM(flat, F32),
            pltpu.VMEM((steps, rounds, width), jnp.int32),
            pltpu.VMEM((owners, rows_here, width), F32),
            pltpu.VMEM((rows_all, width), F32),
            pltpu.VMEM((rows_all if groups == 1 else 2 * width, width), F32),
            pltpu.VMEM((steps, 2, rows_all // 2, half), F32),
            pltpu.VMEM((steps - 1, 2, rows_all // 2, half), F32),
            pltpu.VMEM((rows_all, width), F32),
            pltpu.VMEM((owners, rows_here, width), F32),
            pltpu.VMEM((steps - 1, owners, rows_here, half), F32),
            pltpu.VMEM((steps, owners, rows_here, half), F32),
            pltpu.VMEM((steps, owners, rows_here, half), F32),
            pltpu.VMEM((steps, rounds, owners, 2, half), F32),
            pltpu.VMEM((steps, rounds + 1, width, width), BF16),
            pltpu.VMEM((steps, rounds + 1, 8, width), jnp.int32),
            pltpu.VMEM((steps, groups, width, width) if groups > 1 else (1, 1, 8, 128), F32),
            pltpu.SemaphoreType.REGULAR((1,)), dma((2,)), dma((2,)), dma((owners,)), dma((steps - 1, 2)), dma((steps - 1, 2)),
            dma((steps, groups) if groups > 1 else (1, 1)), dma((steps, groups) if groups > 1 else (1, 1)),
            dma((steps,)), dma((steps, rounds)), dma((steps,)), dma((steps,)), dma((2, steps)),
        ],
        compiler_params=pltpu.CompilerParams(collective_id=0, has_side_effects=True, vmem_limit_bytes=40 << 20),
    )(pltpu.with_memory_space_constraint(matrix.reshape(flat), pltpu.HBM),
      pltpu.with_memory_space_constraint(plan, pltpu.HBM))
    return out.reshape(matrix.shape)


def solution(mesh):
    in_specs = (P("rows", "cols", None, None), P())
    out_specs = P("rows", "cols", None, None)
    sizes = (mesh.shape["rows"], mesh.shape["cols"])
    return jax.shard_map(functools.partial(body, sizes), mesh=mesh, in_specs=in_specs, out_specs=out_specs, check_vma=False)
```

```python
import functools

import jax
import jax.numpy as jnp
from jax import lax
from jax.experimental import pallas as pl
from jax.experimental.pallas import tpu as pltpu
from jax.sharding import PartitionSpec as P

MESH = pl.DeviceIdType.MESH
NN = (((1,), (0,)), ((), ()))
NT = (((1,), (1,)), ((), ()))
F32 = jnp.float32
BF16 = jnp.bfloat16


def dot(a, b, dims=NN, precision=None):
    return lax.dot_general(a, b, dims, precision=precision, preferred_element_type=F32)


def exact_dot(a, b, dims=NN):
    return dot(a, b, dims, lax.Precision.HIGHEST)


def moved_columns(a, onehot):
    hi = a.astype(BF16)
    rest = a - hi.astype(F32)
    mid = rest.astype(BF16)
    lo = (rest - mid.astype(F32)).astype(BF16)
    return dot(hi, onehot) + dot(mid, onehot) + dot(lo, onehot)


def moved_columns_short(a, onehot):
    hi = a.astype(BF16)
    mid = (a - hi.astype(F32)).astype(BF16)
    return dot(hi, onehot) + dot(mid, onehot)


def gathered_columns(a, source):
    rows, width = a.shape
    half = width // 2
    parts = []
    for h in range(2):
        index = source[:, h * half:(h + 1) * half]
        lane = jnp.broadcast_to(index % half, (rows, half))
        second = jnp.broadcast_to(index >= half, (rows, half))
        left, right = (
            jnp.take_along_axis(a[:, k * half:(k + 1) * half], lane, axis=1, mode="promise_in_bounds") for k in range(2))
        parts.append(jnp.where(second, right, left))
    return jnp.concatenate(parts, axis=1)


def rotated_columns(a, cosine, sine):
    half = a.shape[-1] // 2
    left, right = a[..., :half], a[..., half:]
    return jnp.concatenate([cosine * left - sine * right, sine * left + cosine * right], axis=-1)


def folded(a):
    return jnp.sum(a.reshape(-1, 8, a.shape[-1]), axis=0)


def products(factors):
    low = high = cross = 0.0
    for a, b in factors:
        half = a.shape[1] // 2
        low = low + folded(a[:, :half] * b[:, :half])
        high = high + folded(a[:, half:] * b[:, half:])
        cross = cross + folded(a[:, :half] * b[:, half:])
    return low, high, cross


def angles(sums):
    low, high, cross = (jnp.sum(v, axis=0, keepdims=True) for v in sums)
    spread = high - low
    sign = jnp.where(spread >= 0.0, 1.0, -1.0)
    root = jnp.sqrt(spread * spread + 4.0 * cross * cross)
    tangent = sign * 2.0 * cross / (jnp.abs(spread) + root)
    cosine = lax.rsqrt(1.0 + tangent * tangent)
    return cosine, tangent * cosine


def orders(partner):
    width = partner.shape[1]
    shape = (width, width)
    row = lax.broadcasted_iota(jnp.int32, shape, 0)
    col = lax.broadcasted_iota(jnp.int32, shape, 1)
    other = jnp.broadcast_to(partner, shape)
    swap = row == other
    one = jnp.ones(shape, BF16)

    def bits(mask):
        return jnp.where(mask, 1.0, 0.0).astype(BF16)

    swap_b = bits(swap)
    first_row = other > col
    rank_row = dot(bits(first_row), bits(row < col))
    mate_row = dot(rank_row.astype(BF16), swap_b)
    place_row = jnp.where(first_row, rank_row, mate_row + float(width // 2))
    first_col = dot(bits(swap & (col > row)), one) > 0.5
    rank_col = dot(bits(col < row), bits(first_col))
    mate_col = dot(swap_b, rank_col.astype(BF16))
    place_col = jnp.where(first_col, rank_col, mate_col + float(width // 2))
    forward = bits(place_col == col.astype(F32))
    backward = bits(place_row == row.astype(F32))
    return forward, backward


def kernel(sizes, x_hbm, plan_hbm, out_ref, x_ref, plan_ref, stage, held, state, bottoms, landed, tops, row_state,
           row_tops, row_low, row_landed, turns, moves, sources, grams, clear, load_sem, in_send, in_recv, mid_send, mid_recv,
           gram_send, gram_recv, turn_send, turn_recv, row_send, row_recv, direct):
    owners, groups, cols, rows_here, steps, rounds, width = sizes
    half = width // 2
    rows_all = owners * rows_here
    me = lax.axis_index("rows")
    col = lax.axis_index("cols")
    group, mine = me // owners, me % owners
    right = (col + 1) % cols

    def at(owner_shift, col_shift=0, group_shift=0):
        row = ((group + group_shift) % groups) * owners + (mine + owner_shift) % owners
        return row, (col + col_shift) % cols

    peers = {(o, 0, 0) for o in range(owners)} | {(0, c, 0) for c in (1, cols - 1)} | {(0, 0, g) for g in range(groups)}
    peers = sorted(peers - {(0, 0, 0)})
    barrier = pltpu.get_barrier_semaphore()
    for peer in peers:
        pl.semaphore_signal(barrier, inc=1, device_id=at(*peer), device_id_type=MESH)
    load = pltpu.make_async_copy(x_hbm, x_ref, load_sem.at[0])
    load.start()
    load_plan = pltpu.make_async_copy(plan_hbm, plan_ref, load_sem.at[1])
    load_plan.start()
    load.wait()
    for k in range(owners):
        for h in range(2):
            stage[k, :, h * half:(h + 1) * half] = x_ref[pl.ds(2 * k + h, rows_here, stride=2 * owners), :]
    with jax.named_scope("barrier_wait"):
        pl.semaphore_wait(barrier, len(peers))

    def rows_of(owner):
        return pl.ds(pl.multiple_of(owner * rows_here, rows_here), rows_here)

    incoming = {}
    order = sorted(range(1, owners), key=lambda d: (abs(d - owners // 2), d))
    first = owners - 6
    for i, d in enumerate(order):
        incoming[d] = pltpu.make_async_remote_copy(
            stage.at[(mine + d) % owners], held.at[rows_of(mine), :], in_send.at[int(i + 1 >= first)], in_recv.at[d],
            device_id=at(d), device_id_type=MESH)

    def send_rows():
        for d in order:
            incoming[d].start()

    def rows_sent(slot, count):
        sent = stage.at[0:count]
        pltpu.make_async_remote_copy(
            sent, sent, in_send.at[slot], in_recv.at[0], device_id=at(1), device_id_type=MESH).wait_send()

    early = col % 2 == 1
    pl.when(early)(send_rows)
    load_plan.wait()
    ladder = lax.broadcasted_iota(jnp.int32, (8, width), 1).astype(F32).astype(BF16)

    def arrange(s):
        before = None
        for r in range(rounds + 1):
            if r < rounds:
                forward, backward = orders(plan_ref[s, r:r + 1, :])
                move = forward if r == 0 else dot(before, forward).astype(BF16)
                before = backward
            else:
                move = before
            moves[s, r] = move
            sources[s, r] = dot(ladder, move).astype(jnp.int32)

    with jax.named_scope("orders0"):
        arrange(0)

    with jax.named_scope("hand_over"):
        @pl.when(early)
        def _():
            rows_sent(0, first - 1)
            partner = (me, (col + cols - 1) % cols)
            pl.semaphore_signal(clear.at[0], inc=1, device_id=partner, device_id_type=MESH)

        @pl.when(jnp.logical_not(early))
        def _():
            pl.semaphore_wait(clear.at[0], 1)
            send_rows()

    with jax.named_scope("orders1"):
        for s in range(1, steps):
            arrange(s)

    def advanced(ref, turn, s, r):
        parts = []
        cut = ref.shape[0] // 2
        for h in range(2):
            part = ref[h * cut:(h + 1) * cut, :]
            if turn is not None:
                part = rotated_columns(part, *turn)
            if h == 0:
                parts.append(moved_columns(part, moves[s, r]))
            else:
                parts.append(gathered_columns(part, sources[s, r, 0:1, :]))
        return parts

    def kept(ref, parts):
        cut = ref.shape[0] // 2
        for h in range(2):
            ref[h * cut:(h + 1) * cut, :] = parts[h]

    def tell(s, r, turn):
        cosine, sine = turn
        turns[s, r, mine] = jnp.concatenate([cosine, sine], axis=0)
        for d in range(1, owners):
            pltpu.make_async_remote_copy(
                turns.at[s, r, mine], turns.at[s, r, mine], turn_send.at[s], turn_recv.at[s, r],
                device_id=at(d), device_id_type=MESH).start()

    def all_told(s, r):
        block = turns.at[s, r, 0:owners - 1]
        return pltpu.make_async_remote_copy(
            block, block, turn_send.at[s], turn_recv.at[s, r], device_id=at(1), device_id_type=MESH)

    def all_tells(s):
        block = turns.at[s, :, 0:owners - 1]
        return pltpu.make_async_remote_copy(
            block, block, turn_send.at[s], turn_recv.at[s, 0], device_id=at(1), device_id_type=MESH)

    def solved(s, sums):
        if sums is None:
            x = tops[...]
            gram = exact_dot(x.T, x)
            grams[s, group] = gram
            shared = []
            for g in range(1, groups):
                copy = pltpu.make_async_remote_copy(
                    grams.at[s, group], grams.at[s, group], gram_send.at[s, g], gram_recv.at[s, g],
                    device_id=at(0, 0, g), device_id_type=MESH)
                copy.start()
                shared.append(copy)
            for copy in shared:
                copy.wait()
            gram = grams[s, 0]
            for g in range(1, groups):
                gram = gram + grams[s, g]
            state[0:width, :] = gram
            shape = (width, width)
            eye = lax.broadcasted_iota(jnp.int32, shape, 0) == lax.broadcasted_iota(jnp.int32, shape, 1)
            state[width:2 * width, :] = jnp.where(eye, 1.0, 0.0)
        turn, all_turns = None, []
        for r in range(rounds):
            if r > 0 or sums is None:
                parts = advanced(state, turn, s, r)
                kept(state, parts)
                factors = [tuple(parts)] if groups > 1 else [(part, part) for part in parts]
                sums = products(factors)
            turn = angles(sums)
            tell(s, r, turn)
            all_turns.append(turn)
        return all_turns

    def final_parts(s, all_turns):
        if groups > 1:
            turn = None
            for r in range(rounds):
                kept(tops, advanced(tops, turn, s, r))
                turn = all_turns[r]
            return advanced(tops, turn, s, rounds)
        return advanced(state, all_turns[-1], s, rounds)

    chunks = 2
    size = owners // chunks
    side = mine // size

    def near_landed(s, count):
        block = row_landed.at[s, 0:count]
        return pltpu.make_async_remote_copy(
            block, block, direct.at[0, s], direct.at[1, s], device_id=(me, right), device_id_type=MESH)

    def short_moved(q, rows, s, r):
        flat = rows.reshape(size * rows_here, width)
        if q % 2 == 0:
            flat = moved_columns_short(flat, moves[s, r])
        else:
            flat = gathered_columns(flat, sources[s, r, 0:1, :])
        return flat.reshape(size, rows_here, width)

    with jax.named_scope("rows_first"):
        for q in range(chunks):
            part = slice(q * size, (q + 1) * size)
            row_state[part] = short_moved(q, stage[part], 0, 0)

    def first_step(rows):
        if groups > 1:
            tops[rows, :] = held[rows, :]
            return None
        moved = moved_columns(held[rows, :], moves[0, 0])
        state[rows, :] = moved
        return products([(moved, moved)])

    with jax.named_scope("a2a_wait"):
        held[rows_of(mine), :] = stage[mine]
        sums = first_step(rows_of(mine))
        for d in reversed(order):
            incoming[d].wait_recv()
            more = first_step(rows_of((mine + owners - d) % owners))
            if more is not None:
                sums = tuple(a + b for a, b in zip(sums, more))

    cut = rows_all // 2

    def crossing(s, h):
        return pltpu.make_async_remote_copy(
            bottoms.at[s, h], landed.at[s, h], mid_send.at[s, h], mid_recv.at[s, h],
            device_id=(me, right), device_id_type=MESH)

    def passing(s, q=0):
        part = slice(q * size, (q + 1) * size)
        return pltpu.make_async_remote_copy(
            row_low.at[s, part], row_landed.at[s, part], row_send.at[s], row_recv.at[s],
            device_id=(me, right), device_id_type=MESH)

    def solve(s, sums):
        last = s + 1 == steps
        with jax.named_scope(f"solve{s}"):
            all_turns = solved(s, sums)
        with jax.named_scope(f"send{s}"):
            parts = final_parts(s, all_turns)
            for h in range(2):
                bottoms[s, h] = parts[h][:, half:]
                if last:
                    continue
                crossing(s, h).start()
                tops[h * cut:(h + 1) * cut, :half] = parts[h][:, :half]
            for j in range(0 if last else 1, size):
                other = (mine + j) % size
                pltpu.make_async_remote_copy(
                    bottoms.at[s, side, rows_of(other), :], row_landed.at[s, mine], direct.at[0, s], direct.at[1, s],
                    device_id=(group * owners + side * size + other, right), device_id_type=MESH).start()

    def rows_step(s):
        last = s + 1 == steps
        if s > 0:
            with jax.named_scope(f"pass_wait{s}"):
                near_landed(s - 1, size - 1).wait()
                passing(s - 1).wait()
            for q in range(chunks):
                part = slice(q * size, (q + 1) * size)
                rows = jnp.concatenate([row_tops[s - 1, part], row_landed[s - 1, part]], axis=2)
                row_state[part] = short_moved(q, rows, s, 0)
        for r in range(rounds):
            with jax.named_scope(f"told{s}_{r}"):
                all_told(s, r).wait_recv()
            with jax.named_scope(f"turn{s}_{r}"):
                turned = []
                for q in range(chunks):
                    part = slice(q * size, (q + 1) * size)
                    rows = rotated_columns(row_state[part], turns[s, r, part, 0:1, :], turns[s, r, part, 1:2, :])
                    turned.append(short_moved(q, rows, s, r + 1))
                for q in range(chunks):
                    part = slice(q * size, (q + 1) * size)
                    if r + 1 < rounds:
                        row_state[part] = turned[q]
                        continue
                    row_low[s, part] = turned[q][:, :, half:]
                    pl.when(side != q)(passing(s, q).start)
                for q in range(chunks if r + 1 == rounds else 0):
                    part = slice(q * size, (q + 1) * size)
                    if last:
                        for k in range(size):
                            at_rows = pl.ds(2 * (q * size + k), rows_here, stride=2 * owners)
                            out_ref[at_rows, :] = turned[q][k, :, :half]
                    else:
                        row_tops[s, part] = turned[q][:, :, :half]

    def join(s):
        with jax.named_scope(f"cross_wait{s}"):
            for h in range(2):
                crossing(s, h).wait()
        with jax.named_scope(f"cross_join{s}"):
            for h in range(2):
                tops[h * cut:(h + 1) * cut, half:] = landed[s, h]
            row_landed[s, mine] = landed[s, side, rows_of(mine % size), :]
            if groups > 1:
                return None
            parts = advanced(tops, None, s + 1, 0)
            kept(state, parts)
            return products([(part, part) for part in parts])

    solve(0, sums)
    ahead = col % 2 == 0
    for s in range(steps - 1):
        @pl.when(ahead)
        def _():
            solve(s + 1, join(s))
            rows_step(s)

        @pl.when(jnp.logical_not(ahead))
        def _():
            rows_step(s)
            solve(s + 1, join(s))

    rows_step(steps - 1)

    for s in range(steps):
        all_tells(s).wait_send()
    pl.when(jnp.logical_not(early))(functools.partial(rows_sent, 0, first - 1))
    rows_sent(1, owners - first)

    def put_bottoms(q):
        for k in range(q * size, (q + 1) * size):
            out_ref[pl.ds(2 * k + 1, rows_here, stride=2 * owners), :] = row_landed[steps - 1, k]

    with jax.named_scope("direct_wait"):
        near_landed(steps - 1, size).wait()
    for q in range(chunks):
        pl.when(side == q)(functools.partial(put_bottoms, q))
    with jax.named_scope("last_pass"):
        passing(steps - 1).wait()
    for q in range(chunks):
        pl.when(side != q)(functools.partial(put_bottoms, q))


def body(mesh_sizes, matrix, plan):
    rows_here, pair_here, halves, half = matrix.shape
    steps, rounds, width = plan.shape
    rows, cols = mesh_sizes
    owners, groups = pair_here, rows // pair_here
    assert rows % pair_here == 0 and pair_here % 2 == 0 and halves == 2 and cols > 1 and cols % 2 == 0
    sizes = (owners, groups, cols, rows_here, steps, rounds, width)
    dma = pltpu.SemaphoreType.DMA
    rows_all = owners * rows_here
    assert groups == 1 or rows_all >= 2 * width
    flat = (rows_here * pair_here * 2, half)
    anywhere = pl.BlockSpec(memory_space=pltpu.HBM)
    out = pl.pallas_call(
        functools.partial(kernel, sizes),
        out_shape=jax.ShapeDtypeStruct(flat, F32),
        in_specs=[anywhere, anywhere],
        out_specs=pl.BlockSpec(memory_space=pltpu.VMEM),
        scratch_shapes=[
            pltpu.VMEM(flat, F32),
            pltpu.VMEM((steps, rounds, width), jnp.int32),
            pltpu.VMEM((owners, rows_here, width), F32),
            pltpu.VMEM((rows_all, width), F32),
            pltpu.VMEM((rows_all if groups == 1 else 2 * width, width), F32),
            pltpu.VMEM((steps, 2, rows_all // 2, half), F32),
            pltpu.VMEM((steps - 1, 2, rows_all // 2, half), F32),
            pltpu.VMEM((rows_all, width), F32),
            pltpu.VMEM((owners, rows_here, width), F32),
            pltpu.VMEM((steps - 1, owners, rows_here, half), F32),
            pltpu.VMEM((steps, owners, rows_here, half), F32),
            pltpu.VMEM((steps, owners, rows_here, half), F32),
            pltpu.VMEM((steps, rounds, owners, 2, half), F32),
            pltpu.VMEM((steps, rounds + 1, width, width), BF16),
            pltpu.VMEM((steps, rounds + 1, 8, width), jnp.int32),
            pltpu.VMEM((steps, groups, width, width) if groups > 1 else (1, 1, 8, 128), F32),
            pltpu.SemaphoreType.REGULAR((1,)), dma((2,)), dma((2,)), dma((owners,)), dma((steps - 1, 2)), dma((steps - 1, 2)),
            dma((steps, groups) if groups > 1 else (1, 1)), dma((steps, groups) if groups > 1 else (1, 1)),
            dma((steps,)), dma((steps, rounds)), dma((steps,)), dma((steps,)), dma((2, steps)),
        ],
        compiler_params=pltpu.CompilerParams(collective_id=0, has_side_effects=True, vmem_limit_bytes=40 << 20),
    )(pltpu.with_memory_space_constraint(matrix.reshape(flat), pltpu.HBM),
      pltpu.with_memory_space_constraint(plan, pltpu.HBM))
    return out.reshape(matrix.shape)


def solution(mesh):
    in_specs = (P("rows", "cols", None, None), P())
    out_specs = P("rows", "cols", None, None)
    sizes = (mesh.shape["rows"], mesh.shape["cols"])
    return jax.shard_map(functools.partial(body, sizes), mesh=mesh, in_specs=in_specs, out_specs=out_specs, check_vma=False)
```

```python
import functools

import jax
import jax.numpy as jnp
from jax import lax
from jax.experimental import pallas as pl
from jax.experimental.pallas import tpu as pltpu
from jax.sharding import PartitionSpec as P

MESH = pl.DeviceIdType.MESH
NN = (((1,), (0,)), ((), ()))
NT = (((1,), (1,)), ((), ()))
F32 = jnp.float32
BF16 = jnp.bfloat16


def dot(a, b, dims=NN, precision=None):
    return lax.dot_general(a, b, dims, precision=precision, preferred_element_type=F32)


def exact_dot(a, b, dims=NN):
    return dot(a, b, dims, lax.Precision.HIGHEST)


def moved_columns(a, onehot):
    hi = a.astype(BF16)
    rest = a - hi.astype(F32)
    mid = rest.astype(BF16)
    lo = (rest - mid.astype(F32)).astype(BF16)
    return dot(hi, onehot) + dot(mid, onehot) + dot(lo, onehot)


def moved_columns_short(a, onehot):
    hi = a.astype(BF16)
    mid = (a - hi.astype(F32)).astype(BF16)
    return dot(hi, onehot) + dot(mid, onehot)


def gathered_columns(a, source):
    rows, width = a.shape
    half = width // 2
    parts = []
    for h in range(2):
        index = source[:, h * half:(h + 1) * half]
        lane = jnp.broadcast_to(index % half, (rows, half))
        second = jnp.broadcast_to(index >= half, (rows, half))
        left, right = (
            jnp.take_along_axis(a[:, k * half:(k + 1) * half], lane, axis=1, mode="promise_in_bounds") for k in range(2))
        parts.append(jnp.where(second, right, left))
    return jnp.concatenate(parts, axis=1)


def rotated_columns(a, cosine, sine):
    half = a.shape[-1] // 2
    left, right = a[..., :half], a[..., half:]
    return jnp.concatenate([cosine * left - sine * right, sine * left + cosine * right], axis=-1)


def folded(a):
    return jnp.sum(a.reshape(-1, 8, a.shape[-1]), axis=0)


def products(factors):
    low = high = cross = 0.0
    for a, b in factors:
        half = a.shape[1] // 2
        low = low + folded(a[:, :half] * b[:, :half])
        high = high + folded(a[:, half:] * b[:, half:])
        cross = cross + folded(a[:, :half] * b[:, half:])
    return low, high, cross


def angles(sums):
    low, high, cross = (jnp.sum(v, axis=0, keepdims=True) for v in sums)
    spread = high - low
    sign = jnp.where(spread >= 0.0, 1.0, -1.0)
    root = jnp.sqrt(spread * spread + 4.0 * cross * cross)
    tangent = sign * 2.0 * cross / (jnp.abs(spread) + root)
    cosine = lax.rsqrt(1.0 + tangent * tangent)
    return cosine, tangent * cosine


def orders(partner):
    width = partner.shape[1]
    shape = (width, width)
    row = lax.broadcasted_iota(jnp.int32, shape, 0)
    col = lax.broadcasted_iota(jnp.int32, shape, 1)
    other = jnp.broadcast_to(partner, shape)
    swap = row == other
    one = jnp.ones(shape, BF16)

    def bits(mask):
        return jnp.where(mask, 1.0, 0.0).astype(BF16)

    swap_b = bits(swap)
    first_row = other > col
    rank_row = dot(bits(first_row), bits(row < col))
    mate_row = dot(rank_row.astype(BF16), swap_b)
    place_row = jnp.where(first_row, rank_row, mate_row + float(width // 2))
    first_col = dot(bits(swap & (col > row)), one) > 0.5
    rank_col = dot(bits(col < row), bits(first_col))
    mate_col = dot(swap_b, rank_col.astype(BF16))
    place_col = jnp.where(first_col, rank_col, mate_col + float(width // 2))
    forward = bits(place_col == col.astype(F32))
    backward = bits(place_row == row.astype(F32))
    return forward, backward


def kernel(sizes, x_hbm, plan_hbm, out_ref, x_ref, plan_ref, stage, held, state, bottoms, landed, tops, row_state,
           row_tops, row_low, row_landed, turns, moves, sources, grams, clear, load_sem, in_send, in_recv, mid_send, mid_recv,
           gram_send, gram_recv, turn_send, turn_recv, row_send, row_recv, direct):
    owners, groups, cols, rows_here, steps, rounds, width = sizes
    half = width // 2
    rows_all = owners * rows_here
    me = lax.axis_index("rows")
    col = lax.axis_index("cols")
    group, mine = me // owners, me % owners
    right = (col + 1) % cols

    def at(owner_shift, col_shift=0, group_shift=0):
        row = ((group + group_shift) % groups) * owners + (mine + owner_shift) % owners
        return row, (col + col_shift) % cols

    peers = {(o, 0, 0) for o in range(owners)} | {(0, c, 0) for c in (1, cols - 1)} | {(0, 0, g) for g in range(groups)}
    peers = sorted(peers - {(0, 0, 0)})
    barrier = pltpu.get_barrier_semaphore()
    for peer in peers:
        pl.semaphore_signal(barrier, inc=1, device_id=at(*peer), device_id_type=MESH)
    load = pltpu.make_async_copy(x_hbm, x_ref, load_sem.at[0])
    load.start()
    load_plan = pltpu.make_async_copy(plan_hbm, plan_ref, load_sem.at[1])
    load_plan.start()
    load.wait()
    for k in range(owners):
        for h in range(2):
            stage[k, :, h * half:(h + 1) * half] = x_ref[pl.ds(2 * k + h, rows_here, stride=2 * owners), :]
    with jax.named_scope("barrier_wait"):
        pl.semaphore_wait(barrier, len(peers))

    def rows_of(owner):
        return pl.ds(pl.multiple_of(owner * rows_here, rows_here), rows_here)

    incoming = {}
    order = sorted(range(1, owners), key=lambda d: (abs(d - owners // 2), d))
    first = owners - 6
    for i, d in enumerate(order):
        incoming[d] = pltpu.make_async_remote_copy(
            stage.at[(mine + d) % owners], held.at[rows_of(mine), :], in_send.at[int(i + 1 >= first)], in_recv.at[d],
            device_id=at(d), device_id_type=MESH)

    def send_rows():
        for d in order:
            incoming[d].start()

    def rows_sent(slot, count):
        sent = stage.at[0:count]
        pltpu.make_async_remote_copy(
            sent, sent, in_send.at[slot], in_recv.at[0], device_id=at(1), device_id_type=MESH).wait_send()

    early = col % 2 == 1
    pl.when(early)(send_rows)
    load_plan.wait()
    ladder = lax.broadcasted_iota(jnp.int32, (8, width), 1).astype(F32).astype(BF16)

    def arrange(s):
        before = None
        for r in range(rounds + 1):
            if r < rounds:
                forward, backward = orders(plan_ref[s, r:r + 1, :])
                move = forward if r == 0 else dot(before, forward).astype(BF16)
                before = backward
            else:
                move = before
            moves[s, r] = move
            sources[s, r] = dot(ladder, move).astype(jnp.int32)

    with jax.named_scope("orders0"):
        arrange(0)

    with jax.named_scope("hand_over"):
        @pl.when(early)
        def _():
            rows_sent(0, first - 1)
            partner = (me, (col + cols - 1) % cols)
            pl.semaphore_signal(clear.at[0], inc=1, device_id=partner, device_id_type=MESH)

        @pl.when(jnp.logical_not(early))
        def _():
            pl.semaphore_wait(clear.at[0], 1)
            send_rows()

    with jax.named_scope("orders1"):
        for s in range(1, steps):
            arrange(s)

    def advanced(ref, turn, s, r):
        parts = []
        cut = ref.shape[0] // 2
        for h in range(2):
            part = ref[h * cut:(h + 1) * cut, :]
            if turn is not None:
                part = rotated_columns(part, *turn)
            if h == 0:
                parts.append(moved_columns(part, moves[s, r]))
            else:
                parts.append(gathered_columns(part, sources[s, r, 0:1, :]))
        return parts

    def kept(ref, parts):
        cut = ref.shape[0] // 2
        for h in range(2):
            ref[h * cut:(h + 1) * cut, :] = parts[h]

    def tell(s, r, turn):
        cosine, sine = turn
        turns[s, r, mine] = jnp.concatenate([cosine, sine], axis=0)
        for d in range(1, owners):
            pltpu.make_async_remote_copy(
                turns.at[s, r, mine], turns.at[s, r, mine], turn_send.at[s], turn_recv.at[s, r],
                device_id=at(d), device_id_type=MESH).start()

    def all_told(s, r):
        block = turns.at[s, r, 0:owners - 1]
        return pltpu.make_async_remote_copy(
            block, block, turn_send.at[s], turn_recv.at[s, r], device_id=at(1), device_id_type=MESH)

    def all_tells(s):
        block = turns.at[s, :, 0:owners - 1]
        return pltpu.make_async_remote_copy(
            block, block, turn_send.at[s], turn_recv.at[s, 0], device_id=at(1), device_id_type=MESH)

    def solved(s, sums):
        if sums is None:
            x = tops[...]
            gram = exact_dot(x.T, x)
            grams[s, group] = gram
            shared = []
            for g in range(1, groups):
                copy = pltpu.make_async_remote_copy(
                    grams.at[s, group], grams.at[s, group], gram_send.at[s, g], gram_recv.at[s, g],
                    device_id=at(0, 0, g), device_id_type=MESH)
                copy.start()
                shared.append(copy)
            for copy in shared:
                copy.wait()
            gram = grams[s, 0]
            for g in range(1, groups):
                gram = gram + grams[s, g]
            state[0:width, :] = gram
            shape = (width, width)
            eye = lax.broadcasted_iota(jnp.int32, shape, 0) == lax.broadcasted_iota(jnp.int32, shape, 1)
            state[width:2 * width, :] = jnp.where(eye, 1.0, 0.0)
        turn, all_turns = None, []
        for r in range(rounds):
            if r > 0 or sums is None:
                parts = advanced(state, turn, s, r)
                kept(state, parts)
                factors = [tuple(parts)] if groups > 1 else [(part, part) for part in parts]
                sums = products(factors)
            turn = angles(sums)
            tell(s, r, turn)
            all_turns.append(turn)
        return all_turns

    def final_parts(s, all_turns):
        if groups > 1:
            turn = None
            for r in range(rounds):
                kept(tops, advanced(tops, turn, s, r))
                turn = all_turns[r]
            return advanced(tops, turn, s, rounds)
        return advanced(state, all_turns[-1], s, rounds)

    chunks = 2
    size = owners // chunks
    side = mine // size

    def near_landed(s, count):
        block = row_landed.at[s, 0:count]
        return pltpu.make_async_remote_copy(
            block, block, direct.at[0, s], direct.at[1, s], device_id=(me, right), device_id_type=MESH)

    def short_moved(q, rows, s, r):
        flat = rows.reshape(size * rows_here, width)
        if q % 2 == 0:
            flat = moved_columns_short(flat, moves[s, r])
        else:
            flat = gathered_columns(flat, sources[s, r, 0:1, :])
        return flat.reshape(size, rows_here, width)

    with jax.named_scope("rows_first"):
        for q in range(chunks):
            part = slice(q * size, (q + 1) * size)
            row_state[part] = short_moved(q, stage[part], 0, 0)

    def first_step(rows):
        if groups > 1:
            tops[rows, :] = held[rows, :]
            return None
        moved = moved_columns(held[rows, :], moves[0, 0])
        state[rows, :] = moved
        return products([(moved, moved)])

    with jax.named_scope("a2a_wait"):
        held[rows_of(mine), :] = stage[mine]
        sums = first_step(rows_of(mine))
        for d in reversed(order):
            incoming[d].wait_recv()
            more = first_step(rows_of((mine + owners - d) % owners))
            if more is not None:
                sums = tuple(a + b for a, b in zip(sums, more))

    cut = rows_all // 2

    def crossing(s, h):
        return pltpu.make_async_remote_copy(
            bottoms.at[s, h], landed.at[s, h], mid_send.at[s, h], mid_recv.at[s, h],
            device_id=(me, right), device_id_type=MESH)

    def passing(s, q=0):
        part = slice(q * size, (q + 1) * size)
        return pltpu.make_async_remote_copy(
            row_low.at[s, part], row_landed.at[s, part], row_send.at[s], row_recv.at[s],
            device_id=(me, right), device_id_type=MESH)

    def solve(s, sums):
        last = s + 1 == steps
        with jax.named_scope(f"solve{s}"):
            all_turns = solved(s, sums)
        with jax.named_scope(f"send{s}"):
            parts = final_parts(s, all_turns)
            for h in range(2):
                bottoms[s, h] = parts[h][:, half:]
                if last:
                    continue
                crossing(s, h).start()
                tops[h * cut:(h + 1) * cut, :half] = parts[h][:, :half]
            for j in range(0 if last else 1, size):
                other = (mine + j) % size
                pltpu.make_async_remote_copy(
                    bottoms.at[s, side, rows_of(other), :], row_landed.at[s, mine], direct.at[0, s], direct.at[1, s],
                    device_id=(group * owners + side * size + other, right), device_id_type=MESH).start()

    def rows_step(s):
        last = s + 1 == steps
        if s > 0:
            with jax.named_scope(f"pass_wait{s}"):
                near_landed(s - 1, size - 1).wait()
                passing(s - 1).wait()
            for q in range(chunks):
                part = slice(q * size, (q + 1) * size)
                rows = jnp.concatenate([row_tops[s - 1, part], row_landed[s - 1, part]], axis=2)
                row_state[part] = short_moved(q, rows, s, 0)
        for r in range(rounds):
            with jax.named_scope(f"told{s}_{r}"):
                all_told(s, r).wait_recv()
            with jax.named_scope(f"turn{s}_{r}"):
                turned = []
                for q in range(chunks):
                    part = slice(q * size, (q + 1) * size)
                    rows = rotated_columns(row_state[part], turns[s, r, part, 0:1, :], turns[s, r, part, 1:2, :])
                    turned.append(short_moved(q, rows, s, r + 1))
                for q in range(chunks):
                    part = slice(q * size, (q + 1) * size)
                    if r + 1 < rounds:
                        row_state[part] = turned[q]
                        continue

                    @pl.when(side != q)
                    def _():
                        row_low[s, part] = turned[q][:, :, half:]
                        passing(s, q).start()

                for q in range(chunks if r + 1 == rounds else 0):
                    part = slice(q * size, (q + 1) * size)
                    if last:
                        for k in range(size):
                            at_rows = pl.ds(2 * (q * size + k), rows_here, stride=2 * owners)
                            out_ref[at_rows, :] = turned[q][k, :, :half]
                    else:
                        row_tops[s, part] = turned[q][:, :, :half]

    def join(s):
        with jax.named_scope(f"cross_wait{s}"):
            for h in range(2):
                crossing(s, h).wait()
        with jax.named_scope(f"cross_join{s}"):
            for h in range(2):
                tops[h * cut:(h + 1) * cut, half:] = landed[s, h]
            row_landed[s, mine] = landed[s, side, rows_of(mine % size), :]
            if groups > 1:
                return None
            parts = advanced(tops, None, s + 1, 0)
            kept(state, parts)
            return products([(part, part) for part in parts])

    solve(0, sums)
    ahead = col % 2 == 0
    for s in range(steps - 1):
        @pl.when(ahead)
        def _():
            solve(s + 1, join(s))
            rows_step(s)

        @pl.when(jnp.logical_not(ahead))
        def _():
            rows_step(s)
            solve(s + 1, join(s))

    rows_step(steps - 1)

    for s in range(steps):
        all_tells(s).wait_send()
    pl.when(jnp.logical_not(early))(functools.partial(rows_sent, 0, first - 1))
    rows_sent(1, owners - first)

    def put_bottoms(q):
        for k in range(q * size, (q + 1) * size):
            out_ref[pl.ds(2 * k + 1, rows_here, stride=2 * owners), :] = row_landed[steps - 1, k]

    with jax.named_scope("direct_wait"):
        near_landed(steps - 1, size).wait()
    for q in range(chunks):
        pl.when(side == q)(functools.partial(put_bottoms, q))
    with jax.named_scope("last_pass"):
        passing(steps - 1).wait()
    for q in range(chunks):
        pl.when(side != q)(functools.partial(put_bottoms, q))


def body(mesh_sizes, matrix, plan):
    rows_here, pair_here, halves, half = matrix.shape
    steps, rounds, width = plan.shape
    rows, cols = mesh_sizes
    owners, groups = pair_here, rows // pair_here
    assert rows % pair_here == 0 and pair_here % 2 == 0 and halves == 2 and cols > 1 and cols % 2 == 0
    sizes = (owners, groups, cols, rows_here, steps, rounds, width)
    dma = pltpu.SemaphoreType.DMA
    rows_all = owners * rows_here
    assert groups == 1 or rows_all >= 2 * width
    flat = (rows_here * pair_here * 2, half)
    anywhere = pl.BlockSpec(memory_space=pltpu.HBM)
    out = pl.pallas_call(
        functools.partial(kernel, sizes),
        out_shape=jax.ShapeDtypeStruct(flat, F32),
        in_specs=[anywhere, anywhere],
        out_specs=pl.BlockSpec(memory_space=pltpu.VMEM),
        scratch_shapes=[
            pltpu.VMEM(flat, F32),
            pltpu.VMEM((steps, rounds, width), jnp.int32),
            pltpu.VMEM((owners, rows_here, width), F32),
            pltpu.VMEM((rows_all, width), F32),
            pltpu.VMEM((rows_all if groups == 1 else 2 * width, width), F32),
            pltpu.VMEM((steps, 2, rows_all // 2, half), F32),
            pltpu.VMEM((steps - 1, 2, rows_all // 2, half), F32),
            pltpu.VMEM((rows_all, width), F32),
            pltpu.VMEM((owners, rows_here, width), F32),
            pltpu.VMEM((steps - 1, owners, rows_here, half), F32),
            pltpu.VMEM((steps, owners, rows_here, half), F32),
            pltpu.VMEM((steps, owners, rows_here, half), F32),
            pltpu.VMEM((steps, rounds, owners, 2, half), F32),
            pltpu.VMEM((steps, rounds + 1, width, width), BF16),
            pltpu.VMEM((steps, rounds + 1, 8, width), jnp.int32),
            pltpu.VMEM((steps, groups, width, width) if groups > 1 else (1, 1, 8, 128), F32),
            pltpu.SemaphoreType.REGULAR((1,)), dma((2,)), dma((2,)), dma((owners,)), dma((steps - 1, 2)), dma((steps - 1, 2)),
            dma((steps, groups) if groups > 1 else (1, 1)), dma((steps, groups) if groups > 1 else (1, 1)),
            dma((steps,)), dma((steps, rounds)), dma((steps,)), dma((steps,)), dma((2, steps)),
        ],
        compiler_params=pltpu.CompilerParams(collective_id=0, has_side_effects=True, vmem_limit_bytes=40 << 20),
    )(pltpu.with_memory_space_constraint(matrix.reshape(flat), pltpu.HBM),
      pltpu.with_memory_space_constraint(plan, pltpu.HBM))
    return out.reshape(matrix.shape)


def solution(mesh):
    in_specs = (P("rows", "cols", None, None), P())
    out_specs = P("rows", "cols", None, None)
    sizes = (mesh.shape["rows"], mesh.shape["cols"])
    return jax.shard_map(functools.partial(body, sizes), mesh=mesh, in_specs=in_specs, out_specs=out_specs, check_vma=False)
```
